8 devices in a mesh: dp: 2 (over z, y), tp: 4 (over x, core).
Axes of the slice: x: 2, y: 2, z: 1, core: 2. Of those that a mesh axis runs over, the one named last changes fastest.
Arguments:
- hidden: bfloat16 [128, 5120], P('dp'), parts along dimension 0
- cache_len: int32 [128], P('dp'), parts along dimension 0
- lin_state: float32 [128, 32, 128, 128], P('dp', 'tp'), parts along dimension 0
- k_cache: bfloat16 [128, 8, 512, 128], P('dp', 'tp'), parts along dimension 0
- v_cache: bfloat16 [128, 8, 512, 128], P('dp', 'tp'), parts along dimension 0
- norm_first: float32 [5120], replicated
- w_qkv: bfloat16 [5120, 3, 32, 128], P(None, None, 'tp')
- w_gate: bfloat16 [5120, 32, 128], P(None, 'tp')
- slopes: float32 [32], P('tp')
- out_norm: float32 [32, 128], P('tp')
- w_out_lin: bfloat16 [32, 128, 5120], P('tp')
- norm_second: float32 [5120], replicated
- w_attn: bfloat16 [5120, 8, 6, 128], P(None, 'tp')
- w_out_attn: bfloat16 [32, 128, 5120], P('tp')
- mix_alpha: float32 [2], replicated
- mix_beta: float32 [2], replicated
Outputs:
- output 1: bfloat16 [128, 5120], P('dp'), parts along dimension 0
- output 2: float32 [128, 32, 128, 128], P('dp', 'tp'), parts along dimension 0
- output 3: bfloat16 [128, 8, 512, 128], P('dp', 'tp'), parts along dimension 0
- output 4: bfloat16 [128, 8, 512, 128], P('dp', 'tp'), parts along dimension 0
There are 2 independent parts. The reference program is written for one: setup_inputs(seed, part) draws one part's arguments, and reference() takes and returns one part's arrays. A program takes and returns all parts, laid end to end along the dimension named above; an argument that names none is the same for every part.
All inputs are finite; a program needn't handle non-finite values.
Results may differ from the reference program's by a relative error of at most 0.0113869.
Values sent between devices are 32-bit elements.
A program may use at most 1 GiB of HBM per device.

```python
import math
import jax
import jax.numpy as jnp
from jax import lax

D = 5120
HEADS = 32
KV_HEADS = 8
HEAD = 128
BATCH = 64
TMAX = 512

GROUP = HEADS // KV_HEADS
WIDTH = HEADS * HEAD
LEN_MIN = TMAX // 16
EPS = 1e-5
ROPE_BASE = 10000000.0


def setup_inputs(seed: int = 0, part: int = 0) -> dict:
    shared_keys = jax.random.split(jax.random.key(seed), 11)
    own_keys = jax.random.split(jax.random.fold_in(jax.random.key(seed), part), 8)
    hidden = jax.random.normal(own_keys[0], (BATCH, D), jnp.float32).astype(jnp.bfloat16)
    cache_len = jax.random.randint(own_keys[1], (BATCH,), LEN_MIN, TMAX, jnp.int32)
    cache_len = cache_len.at[0].set(TMAX - 1).at[1].set(LEN_MIN)
    head_scale = jnp.exp(jax.random.uniform(own_keys[2], (BATCH, HEADS, 1, 1), jnp.float32, -1.0, 1.0))
    lin_state = 2.0 * head_scale * jax.random.normal(own_keys[3], (BATCH, HEADS, HEAD, HEAD), jnp.float32)
    key_scale = math.sqrt(math.log(TMAX / 32.0))
    k_cache = (key_scale * jax.random.normal(own_keys[4], (BATCH, KV_HEADS, TMAX, HEAD), jnp.float32)).astype(jnp.bfloat16)
    pos_ramp = (2.0 * jnp.arange(TMAX, dtype=jnp.float32) / TMAX - 1.0)[None, None, :, None]
    v_base = jax.random.normal(own_keys[5], (BATCH, KV_HEADS, 1, HEAD), jnp.float32)
    v_slope = jax.random.normal(own_keys[6], (BATCH, KV_HEADS, 1, HEAD), jnp.float32)
    v_noise = jax.random.normal(own_keys[7], (BATCH, KV_HEADS, TMAX, HEAD), jnp.float32)
    v_cache = (0.5 * v_base + 0.5 * v_slope * pos_ramp + v_noise).astype(jnp.bfloat16)
    norm_first = jax.random.uniform(shared_keys[0], (D,), jnp.float32, 0.5, 1.5)
    w_qkv = (jax.random.normal(shared_keys[1], (D, 3, HEADS, HEAD), jnp.float32) * D ** -0.5).astype(jnp.bfloat16)
    w_gate = (jax.random.normal(shared_keys[2], (D, HEADS, HEAD), jnp.float32) * D ** -0.5).astype(jnp.bfloat16)
    slopes = jax.random.uniform(shared_keys[3], (HEADS,), jnp.float32, 0.02, 0.3)
    out_norm = jax.random.uniform(shared_keys[4], (HEADS, HEAD), jnp.float32, 0.5, 1.5)
    w_out_lin = (jax.random.normal(shared_keys[5], (HEADS, HEAD, D), jnp.float32) * WIDTH ** -0.5).astype(jnp.bfloat16)
    norm_second = jax.random.uniform(shared_keys[6], (D,), jnp.float32, 0.5, 1.5)
    w_attn = (jax.random.normal(shared_keys[7], (D, KV_HEADS, GROUP + 2, HEAD), jnp.float32) * D ** -0.5).astype(jnp.bfloat16)
    w_out_attn = (jax.random.normal(shared_keys[8], (HEADS, HEAD, D), jnp.float32) * WIDTH ** -0.5).astype(jnp.bfloat16)
    mix_alpha = jax.random.uniform(shared_keys[9], (2,), jnp.float32, 0.5, 1.5)
    mix_beta = jax.random.uniform(shared_keys[10], (2,), jnp.float32, 0.5, 1.5)
    return dict(hidden=hidden, cache_len=cache_len, lin_state=lin_state, k_cache=k_cache, v_cache=v_cache,
                norm_first=norm_first, w_qkv=w_qkv, w_gate=w_gate, slopes=slopes, out_norm=out_norm,
                w_out_lin=w_out_lin, norm_second=norm_second, w_attn=w_attn, w_out_attn=w_out_attn,
                mix_alpha=mix_alpha, mix_beta=mix_beta)


def rms_norm(values, gain_vec):
    wide_vals = values.astype(jnp.float32)
    mean_sq = jnp.mean(wide_vals * wide_vals, axis=-1, keepdims=True)
    return wide_vals * lax.rsqrt(mean_sq + EPS) * gain_vec


def rotary(values, positions):
    rot_dim = values.shape[-1] // 2
    half_dim = rot_dim // 2
    inv_freq = ROPE_BASE ** (-2.0 * jnp.arange(half_dim, dtype=jnp.float32) / rot_dim)
    angles = positions.astype(jnp.float32)[:, None] * inv_freq[None, :]
    cosine = jnp.cos(angles)[:, None, None, :]
    sine_val = jnp.sin(angles)[:, None, None, :]
    rot_first = values[..., :half_dim]
    rot_second = values[..., half_dim:rot_dim]
    return jnp.concatenate([rot_first * cosine - rot_second * sine_val,
                            rot_second * cosine + rot_first * sine_val,
                            values[..., rot_dim:]], axis=-1)


def lightning_layer(h_first, lin_state, w_qkv, w_gate, slopes, out_norm, w_out_lin):
    proj_lin = jnp.dot(h_first, w_qkv.reshape(D, 3 * WIDTH), preferred_element_type=jnp.float32)
    proj_lin = jax.nn.silu(proj_lin).astype(jnp.bfloat16).astype(jnp.float32).reshape(BATCH, 3, HEADS, HEAD)
    query_lin = proj_lin[:, 0]
    key_lin = proj_lin[:, 1]
    value_lin = proj_lin[:, 2]
    decay_rate = jnp.exp(-slopes)[None, :, None, None]
    state_out = decay_rate * lin_state + jnp.einsum('bhk,bhv->bhkv', key_lin, value_lin)
    lin_attn = jnp.einsum('bhk,bhkv->bhv', query_lin, state_out)
    mean_sq = jnp.mean(lin_attn * lin_attn, axis=(1, 2), keepdims=True)
    normed = (lin_attn * lax.rsqrt(mean_sq + EPS) * out_norm).reshape(BATCH, WIDTH)
    gate_val = jax.nn.sigmoid(jnp.dot(h_first, w_gate.reshape(D, WIDTH), preferred_element_type=jnp.float32))
    gated_out = (normed * gate_val).astype(jnp.bfloat16)
    lin_out = jnp.dot(gated_out, w_out_lin.reshape(WIDTH, D), preferred_element_type=jnp.float32)
    return lin_out, state_out


def softmax_layer(h_second, cache_len, k_cache, v_cache, w_attn, w_out_attn):
    proj_attn = jnp.dot(h_second, w_attn.reshape(D, KV_HEADS * (GROUP + 2) * HEAD), preferred_element_type=jnp.float32)
    proj_attn = proj_attn.reshape(BATCH, KV_HEADS, GROUP + 2, HEAD)
    turned = rotary(proj_attn[:, :, :GROUP + 1], cache_len).astype(jnp.bfloat16)
    query_new = turned[:, :, :GROUP]
    key_new = turned[:, :, GROUP]
    value_new = proj_attn[:, :, GROUP + 1].astype(jnp.bfloat16)
    positions = jnp.arange(TMAX, dtype=jnp.int32)
    write_mask = (positions[None, :] == cache_len[:, None])[:, None, :, None]
    k_out = jnp.where(write_mask, key_new[:, :, None, :], k_cache)
    v_out = jnp.where(write_mask, value_new[:, :, None, :], v_cache)

    def one_row(row_args):
        query_row, key_row, value_row, length = row_args
        scores = jnp.einsum('kgc,ktc->kgt', query_row.astype(jnp.float32), key_row.astype(jnp.float32)) * HEAD ** -0.5
        scores = jnp.where(positions[None, None, :] <= length, scores, -jnp.inf)
        probs_row = jax.nn.softmax(scores, axis=-1).astype(jnp.bfloat16)
        return jnp.einsum('kgt,ktc->kgc', probs_row.astype(jnp.float32), value_row.astype(jnp.float32)).astype(jnp.bfloat16)

    attn_rows = lax.map(one_row, (query_new, k_out, v_out, cache_len))
    attn_out = jnp.dot(attn_rows.reshape(BATCH, WIDTH), w_out_attn.reshape(WIDTH, D), preferred_element_type=jnp.float32)
    return attn_out, k_out, v_out


def reference(hidden, cache_len, lin_state, k_cache, v_cache, norm_first, w_qkv, w_gate, slopes, out_norm,
              w_out_lin, norm_second, w_attn, w_out_attn, mix_alpha, mix_beta):
    h_first = rms_norm(hidden, norm_first).astype(jnp.bfloat16)
    lin_out, state_out = lightning_layer(h_first, lin_state, w_qkv, w_gate, slopes, out_norm, w_out_lin)
    mid_hidden = (mix_alpha[0] * h_first.astype(jnp.float32) + mix_beta[0] * lin_out).astype(jnp.bfloat16)
    h_second = rms_norm(mid_hidden, norm_second).astype(jnp.bfloat16)
    attn_out, k_out, v_out = softmax_layer(h_second, cache_len, k_cache, v_cache, w_attn, w_out_attn)
    hidden_out = (mix_alpha[1] * h_second.astype(jnp.float32) + mix_beta[1] * attn_out).astype(jnp.bfloat16)
    return hidden_out, state_out, k_out, v_out
```

```python
import functools
import jax
import jax.numpy as jnp
from jax import lax
from jax.experimental import pallas as pl
from jax.experimental.pallas import tpu as pltpu
from jax.sharding import PartitionSpec as P

EPS = 1e-5
ROPE_BASE = 10000000.0
F32 = jnp.float32
BF16 = jnp.bfloat16
MESH = pl.DeviceIdType.MESH
ANY = pl.BlockSpec(memory_space=pl.ANY)
VMEM = pl.BlockSpec(memory_space=pltpu.VMEM)
SMEM = pl.BlockSpec(memory_space=pltpu.SMEM)

DC = 256
RS = 9 * DC + 16
NWB = 4
NSB = 16
LAG = 4


def k1_body(hid, g1, wqkv, wgate, slopes, lin, st_out, o_out, gate_out, h1_out,
            wbuf, gbuf, scr, acc, qt, kt, vv, sbuf, wsem, rsem, ssem):
    nchunk = hid.shape[1] // DC

    def wcopies(i, slot):
        return (pltpu.make_async_copy(wqkv.at[pl.ds(i * (DC * 24), DC * 24)], wbuf.at[slot], wsem.at[slot, 0]),
                pltpu.make_async_copy(wgate.at[pl.ds(i * (DC * 8), DC * 8)], gbuf.at[slot], wsem.at[slot, 1]))

    def sread(j, slot):
        hp, bb = j // 8, lax.rem(j, 8)
        return pltpu.make_async_copy(lin.at[pl.ds(bb * 8, 8), pl.ds(hp * 2, 2)], sbuf.at[slot], rsem.at[slot])

    def swrite(j, slot):
        hp, bb = j // 8, lax.rem(j, 8)
        return pltpu.make_async_copy(sbuf.at[slot], st_out.at[pl.ds(bb * 8, 8), pl.ds(hp * 2, 2)], ssem.at[slot])

    for i in range(NWB):
        for c in wcopies(i, i):
            c.start()
    x = hid[...].astype(F32)
    h1_out[...] = (x * lax.rsqrt(jnp.mean(x * x, axis=-1, keepdims=True) + EPS) * g1[...]).astype(BF16)
    acc[...] = jnp.zeros_like(acc)

    def wstep(i, carry):
        slot = lax.rem(i, NWB)
        for c in wcopies(i, slot):
            c.wait()
        for d2 in range(0, DC, 2):
            t = wbuf[slot, pl.ds(d2 * 24, 48)].astype(F32)
            for u in range(6):
                scr[pl.ds((u % 3) * RS + 9 * (d2 + u // 3), 8, stride=2)] = t[u * 8:(u + 1) * 8]
            t = gbuf[slot, pl.ds(d2 * 8, 16)].astype(F32)
            for u in range(2):
                scr[pl.ds(3 * RS + 9 * (d2 + u), 8, stride=2)] = t[u * 8:(u + 1) * 8]
        hh = h1_out[:, pl.ds(pl.multiple_of(i * DC, DC), DC)]

        def head(m):
            return scr[pl.ds((m // 8) * RS + 2 * (m % 8), DC, stride=9)]

        for n in range(16):
            r = jnp.concatenate([head(2 * n), head(2 * n + 1)], axis=1).astype(BF16)
            acc[:, n * 256:(n + 1) * 256] += jnp.dot(hh, r, preferred_element_type=F32)

        @pl.when(i + NWB < nchunk)
        def _():
            for c in wcopies(i + NWB, slot):
                c.start()

        @pl.when(i < NSB)
        def _():
            sread(i, i).start()
        return carry

    lax.fori_loop(0, nchunk, wstep, 0)

    for hp in range(4):
        def pair(c):
            base = c * 1024 + hp * 256
            return jnp.concatenate([acc[:, base:base + 128], acc[:, base + 128:base + 256]], axis=0)

        def act(c):
            z = pair(c)
            return (z * jax.nn.sigmoid(z)).astype(BF16).astype(F32)
        qt[hp] = act(0).T
        kt[hp] = act(1).T
        vv[hp] = act(2)
        g = jax.nn.sigmoid(pair(3))
        gate_out[2 * hp] = g[:64]
        gate_out[2 * hp + 1] = g[64:]

    def sstep(j, carry):
        hp, bb = j // 8, lax.rem(j, 8)
        slot = lax.rem(j, NSB)
        sread(j, slot).wait()
        shift = lax.rem(128 - bb * 8, 128)
        qr = pltpu.roll(qt[hp], shift, 1)
        kr = pltpu.roll(kt[hp], shift, 1)
        for p in range(2):
            decay = jnp.exp(jnp.full((8, 128), -slopes[hp * 2 + p], F32))[0:1]
            vrows = vv[hp, pl.ds(p * 64 + bb * 8, 8)]
            rows = []
            for i in range(8):
                col = p * 64 + i
                kc = jnp.broadcast_to(kr[:, col:col + 1], (128, 128))
                qc = jnp.broadcast_to(qr[:, col:col + 1], (128, 128))
                s_new = decay * sbuf[slot, i, p] + kc * vrows[i:i + 1]
                sbuf[slot, i, p] = s_new
                rows.append(jnp.sum(qc * s_new, axis=0, keepdims=True))
            o_out[hp * 2 + p, pl.ds(bb * 8, 8)] = jnp.concatenate(rows, axis=0)
        swrite(j, slot).start()

        @pl.when((j >= LAG) & (j - LAG + NSB < 32))
        def _():
            jj = j - LAG
            ps = lax.rem(jj, NSB)
            swrite(jj, ps).wait()
            sread(jj + NSB, ps).start()
        return carry

    lax.fori_loop(0, 32, sstep, 0)
    for j in range(32 - NSB, 32):
        swrite(j, j % NSB).wait()


def k1(hidden, g1, wqkv, wgate, slopes, lin):
    return pl.pallas_call(
        k1_body,
        out_shape=(jax.ShapeDtypeStruct(lin.shape, F32), jax.ShapeDtypeStruct((8, 64, 128), F32),
                   jax.ShapeDtypeStruct((8, 64, 128), F32), jax.ShapeDtypeStruct(hidden.shape, BF16)),
        in_specs=[VMEM, VMEM, ANY, ANY, SMEM, ANY],
        out_specs=(ANY, VMEM, VMEM, VMEM),
        scratch_shapes=[
            pltpu.VMEM((NWB, DC * 24, 128), BF16), pltpu.VMEM((NWB, DC * 8, 128), BF16),
            pltpu.VMEM((4 * RS, 128), F32), pltpu.VMEM((64, 4096), F32),
            pltpu.VMEM((4, 128, 128), F32), pltpu.VMEM((4, 128, 128), F32), pltpu.VMEM((4, 128, 128), F32),
            pltpu.VMEM((NSB, 8, 2, 128, 128), F32),
            pltpu.SemaphoreType.DMA((NWB, 2)), pltpu.SemaphoreType.DMA((NSB,)), pltpu.SemaphoreType.DMA((NSB,))],
        compiler_params=pltpu.CompilerParams(vmem_limit_bytes=50 * 2 ** 20),
        name='lightning')(hidden, g1, wqkv, wgate, slopes, lin)


NCH = 5
CW = 512
HALF = NCH * CW


def entry_barrier():
    tp = lax.axis_index('tp')
    bar = pltpu.get_barrier_semaphore()
    for peer in peers(tp):
        pl.semaphore_signal(bar, inc=1, device_id={'tp': peer}, device_id_type=MESH)
    pl.semaphore_wait(bar, 3)


def peers(tp):
    core = lax.rem(tp, 2)
    partner = tp + 1 - 2 * core
    across = lax.rem(tp + 2, 4)
    diag = lax.rem(partner + 2, 4)
    return partner, across, diag


def out_weight_copies(w, wo, wosem):
    core = lax.rem(lax.axis_index('tp'), 2)
    out = []
    for s in range(2 * NCH):
        side = core if s % 2 else 1 - core
        col = pl.multiple_of(side * HALF + (s // 2) * CW, CW)
        out.append(pltpu.make_async_copy(w.at[:, pl.ds(col, CW)], wo.at[s], wosem.at[s]))
    return out


def reduce_over_tp(xin, wo, wcopies, full, send_a, recv_a, own, recv_x, sems, between):
    tp = lax.axis_index('tp')
    core = lax.rem(tp, 2)
    partner, across, _ = peers(tp)

    def rcopy(src, dst, k, j, dev):
        return pltpu.make_async_remote_copy(src_ref=src, dst_ref=dst, send_sem=sems.at[k, j],
                                            recv_sem=sems.at[k + 1, j], device_id={'tp': dev}, device_id_type=MESH)
    ca = [rcopy(send_a.at[j], recv_a.at[j], 0, j, partner) for j in range(NCH)]
    cx = [rcopy(own.at[j], recv_x.at[j], 2, j, across) for j in range(NCH)]
    cf = []
    for j in range(NCH):
        col = pl.multiple_of(core * HALF + j * CW, CW)
        cf.append(rcopy(full.at[:, pl.ds(col, CW)], full.at[:, pl.ds(col, CW)], 4, j, partner))

    def combine(j):
        ca[j].wait_recv()
        own[j] = own[j] + recv_a[j]
        cx[j].start()

    for j in range(NCH):
        wcopies[2 * j].wait()
        send_a[j] = jnp.dot(xin[...], wo[2 * j], preferred_element_type=F32)
        ca[j].start()
        wcopies[2 * j + 1].wait()
        own[j] = jnp.dot(xin[...], wo[2 * j + 1], preferred_element_type=F32)
        if j:
            combine(j - 1)
    combine(NCH - 1)
    for j in range(NCH):
        between(j)
        cx[j].wait_recv()
        col = pl.multiple_of(core * HALF + j * CW, CW)
        full[:, pl.ds(col, CW)] = own[j] + recv_x[j]
        cf[j].start()
    for j in range(NCH):
        cf[j].wait_recv()
    for j in range(NCH):
        ca[j].wait_send()
        cx[j].wait_send()
        cf[j].wait_send()


REDUCE_SCRATCH = [
    pltpu.VMEM((64, 2 * HALF), F32), pltpu.VMEM((NCH, 64, CW), F32), pltpu.VMEM((NCH, 64, CW), F32),
    pltpu.VMEM((NCH, 64, CW), F32), pltpu.VMEM((NCH, 64, CW), F32),
    pltpu.VMEM((2 * NCH, 1024, CW), BF16), pltpu.SemaphoreType.DMA((6, NCH)), pltpu.SemaphoreType.DMA((2 * NCH,))]

NAB = 4


def k2_body(o_in, gate_in, h1, onorm, w_out, g2, wattn, cosf, sina, sinb, alpha, beta,
            h2_out, qs, kn, vn,
            full, send_a, recv_a, own, recv_x, wo, sems, wosem,
            xin, ssl, ssr, sssem, abuf, ascr, wd, asem):
    tp = lax.axis_index('tp')
    nchunk = h1.shape[1] // DC
    wcopies = out_weight_copies(w_out, wo, wosem)
    for c in wcopies:
        c.start()

    def acopy(i, slot):
        return pltpu.make_async_copy(wattn.at[pl.ds(i * (DC * 12), DC * 12)], abuf.at[slot], asem.at[slot])
    for i in range(NAB):
        acopy(i, i).start()
    sq = jnp.zeros((64, 128), F32)
    for h in range(8):
        sq = sq + o_in[h] * o_in[h]
    ssl[...] = sq
    entry_barrier()
    copies = [pltpu.make_async_remote_copy(src_ref=ssl, dst_ref=ssr.at[k], send_sem=sssem.at[0, k],
                                           recv_sem=sssem.at[1, k], device_id={'tp': dev}, device_id_type=MESH)
              for k, dev in enumerate(peers(tp))]
    for c in copies:
        c.start()
    for c in copies:
        c.wait_recv()
    total = jnp.sum((ssl[...] + ssr[0]) + (ssr[1] + ssr[2]), axis=-1, keepdims=True)
    inv = lax.rsqrt(total / 4096.0 + EPS)
    for h in range(8):
        xin[:, h * 128:(h + 1) * 128] = (o_in[h] * inv * onorm[h:h + 1] * gate_in[h]).astype(BF16)

    def demix(i, carry):
        slot = lax.rem(i, NAB)
        acopy(i, slot).wait()
        ascr[...] = abuf[slot].astype(F32)
        for j in range(6):
            for kv in range(2):
                wd[j, kv, pl.ds(pl.multiple_of(i * DC, DC), DC)] = ascr[pl.ds(2 * j + kv, DC, stride=12)].astype(BF16)

        @pl.when(i + NAB < nchunk)
        def _():
            acopy(i + NAB, slot).start()
        return carry

    def between(j):
        lax.fori_loop(j * (nchunk // NCH), (j + 1) * (nchunk // NCH), demix, 0)

    reduce_over_tp(xin, wo, wcopies, full, send_a, recv_a, own, recv_x, sems, between)
    for c in copies:
        c.wait_send()
    mid = (alpha[0] * h1[...].astype(F32) + beta[0] * full[...]).astype(BF16).astype(F32)
    h2_out[...] = (mid * lax.rsqrt(jnp.mean(mid * mid, axis=-1, keepdims=True) + EPS) * g2[...]).astype(BF16)
    qs[...] = jnp.zeros_like(qs)

    def turn(z):
        return z * cosf[...] + pltpu.roll(z, 96, 1) * sina[...] + pltpu.roll(z, 32, 1) * sinb[...]

    for j in range(6):
        r = jnp.concatenate([wd[j, 0], wd[j, 1]], axis=1)
        z = jnp.dot(h2_out[...], r, preferred_element_type=F32)
        for kv in range(2):
            zk = z[:, kv * 128:(kv + 1) * 128]
            if j < 4:
                qs[kv, pl.ds(kv * 4 + j, 64, stride=8)] = turn(zk).astype(BF16).astype(F32)
            elif j == 4:
                kn[kv] = turn(zk).astype(BF16).astype(F32)
            else:
                vn[kv] = zk.astype(BF16).astype(F32)


def k2(o, gate, h1, onorm, w_out, g2, wattn, cosf, sina, sinb, alpha, beta):
    return pl.pallas_call(
        k2_body,
        out_shape=(jax.ShapeDtypeStruct(h1.shape, BF16), jax.ShapeDtypeStruct((2, 512, 128), F32),
                   jax.ShapeDtypeStruct((2, 64, 128), F32), jax.ShapeDtypeStruct((2, 64, 128), F32)),
        in_specs=[VMEM, VMEM, VMEM, VMEM, ANY, VMEM, ANY, VMEM, VMEM, VMEM, SMEM, SMEM],
        out_specs=(VMEM, VMEM, VMEM, VMEM),
        scratch_shapes=REDUCE_SCRATCH + [
            pltpu.VMEM((64, 1024), BF16), pltpu.VMEM((64, 128), F32), pltpu.VMEM((3, 64, 128), F32),
            pltpu.SemaphoreType.DMA((2, 3)),
            pltpu.VMEM((NAB, DC * 12, 128), BF16), pltpu.VMEM((DC * 12, 128), F32),
            pltpu.VMEM((6, 2, h1.shape[1], 128), BF16), pltpu.SemaphoreType.DMA((NAB,))],
        compiler_params=pltpu.CompilerParams(vmem_limit_bytes=50 * 2 ** 20, collective_id=0, has_side_effects=True),
        name='mix_first')(o, gate, h1, onorm, w_out, g2, wattn, cosf, sina, sinb, alpha, beta)


NB3 = 4
NS3 = 5


def k3_body(kc, vc, qs, kn, vn, clen, k_out, v_out, attn, kb, vb, rsem, wsem):
    nstep = kc.shape[0] // NB3

    def reads(i, slot):
        return (pltpu.make_async_copy(kc.at[pl.ds(i * NB3, NB3)], kb.at[slot], rsem.at[slot, 0]),
                pltpu.make_async_copy(vc.at[pl.ds(i * NB3, NB3)], vb.at[slot], rsem.at[slot, 1]))

    def writes(i, slot):
        return (pltpu.make_async_copy(kb.at[slot], k_out.at[pl.ds(i * NB3, NB3)], wsem.at[slot, 0]),
                pltpu.make_async_copy(vb.at[slot], v_out.at[pl.ds(i * NB3, NB3)], wsem.at[slot, 1]))

    for i in range(NS3 - 1):
        for c in reads(i, i):
            c.start()

    def step(i, carry):
        slot = lax.rem(i, NS3)
        for c in reads(i, slot):
            c.wait()
        row_id = lax.broadcasted_iota(jnp.int32, (16, 128), 0)
        for u in range(NB3):
            b = i * NB3 + u
            pos = clen[b]
            base = pl.multiple_of((pos // 16) * 16, 16)
            hit = row_id == pos - base
            for kv in range(2):
                for buf, new in ((kb, kn), (vb, vn)):
                    old = buf[slot, u, kv, pl.ds(base, 16)].astype(F32)
                    row = jnp.broadcast_to(new[kv, pl.ds(b, 1)], (16, 128))
                    buf[slot, u, kv, pl.ds(base, 16)] = jnp.where(hit, row, old).astype(BF16)
        for c in writes(i, slot):
            c.start()
        tpos = lax.broadcasted_iota(jnp.int32, (8, 512), 1)
        lo = lax.broadcasted_iota(jnp.int32, (8, 128), 0) < 4
        for u in range(NB3):
            b = i * NB3 + u
            q = jnp.concatenate([qs[0, pl.ds(b * 8, 8)], qs[1, pl.ds(b * 8, 8)]], axis=1).astype(BF16)
            kk = jnp.concatenate([kb[slot, u, 0], kb[slot, u, 1]], axis=1)
            vvv = jnp.concatenate([vb[slot, u, 0], vb[slot, u, 1]], axis=1)
            s = lax.dot_general(q, kk, (((1,), (1,)), ((), ())), preferred_element_type=F32) * (128 ** -0.5)
            s = jnp.where(tpos <= clen[b], s, -jnp.inf)
            e = jnp.exp(s - jnp.max(s, axis=-1, keepdims=True))
            pr = (e / jnp.sum(e, axis=-1, keepdims=True)).astype(BF16)
            r = jnp.dot(pr, vvv, preferred_element_type=F32)
            attn[pl.ds(b * 8, 8)] = jnp.where(lo, r[:, :128], r[:, 128:]).astype(BF16).astype(F32)

        nxt = i + NS3 - 1

        @pl.when(nxt < nstep)
        def _():
            ps = lax.rem(nxt, NS3)

            @pl.when(i >= 1)
            def _():
                for c in writes(i - 1, ps):
                    c.wait()
            for c in reads(nxt, ps):
                c.start()
        return carry

    lax.fori_loop(0, nstep, step, 0)
    for i in range(nstep - NS3, nstep):
        for c in writes(i, i % NS3):
            c.wait()


def k3(kc, vc, qs, kn, vn, clen):
    shape = (NS3, NB3) + kc.shape[1:]
    return pl.pallas_call(
        k3_body,
        out_shape=(jax.ShapeDtypeStruct(kc.shape, BF16), jax.ShapeDtypeStruct(vc.shape, BF16),
                   jax.ShapeDtypeStruct((512, 128), F32)),
        in_specs=[ANY, ANY, VMEM, VMEM, VMEM, SMEM],
        out_specs=(ANY, ANY, VMEM),
        scratch_shapes=[pltpu.VMEM(shape, BF16), pltpu.VMEM(shape, BF16),
                        pltpu.SemaphoreType.DMA((NS3, 2)), pltpu.SemaphoreType.DMA((NS3, 2))],
        compiler_params=pltpu.CompilerParams(vmem_limit_bytes=50 * 2 ** 20),
        name='attention')(kc, vc, qs, kn, vn, clen)


def k4_body(attn, h2, w_out, alpha, beta, out,
            full, send_a, recv_a, own, recv_x, wo, sems, wosem, xin):
    wcopies = out_weight_copies(w_out, wo, wosem)
    for c in wcopies:
        c.start()
    for r in range(8):
        xin[:, r * 128:(r + 1) * 128] = attn[pl.ds(r, 64, stride=8)].astype(BF16)
    entry_barrier()
    reduce_over_tp(xin, wo, wcopies, full, send_a, recv_a, own, recv_x, sems, lambda j: None)
    out[...] = (alpha[1] * h2[...].astype(F32) + beta[1] * full[...]).astype(BF16)


def k4(attn, h2, w_out, alpha, beta):
    return pl.pallas_call(
        k4_body,
        out_shape=jax.ShapeDtypeStruct(h2.shape, BF16),
        in_specs=[VMEM, VMEM, ANY, SMEM, SMEM],
        out_specs=VMEM,
        scratch_shapes=REDUCE_SCRATCH + [pltpu.VMEM((64, 1024), BF16)],
        compiler_params=pltpu.CompilerParams(vmem_limit_bytes=50 * 2 ** 20, collective_id=1, has_side_effects=True),
        name='mix_second')(attn, h2, w_out, alpha, beta)


def rope_tables(clen):
    inv_freq = ROPE_BASE ** (-2.0 * jnp.arange(32, dtype=F32) / 64)
    ang = clen.astype(F32)[:, None] * inv_freq[None, :]
    cos, sin = jnp.cos(ang), jnp.sin(ang)
    zero = jnp.zeros((clen.shape[0], 32), F32)
    one = jnp.ones((clen.shape[0], 64), F32)
    cosf = jnp.concatenate([cos, cos, one], axis=1)
    sina = jnp.concatenate([-sin, zero, zero, zero], axis=1)
    sinb = jnp.concatenate([zero, sin, zero, zero], axis=1)
    return cosf, sina, sinb


def solution(mesh):
    row_spec = P('dp', None)
    cache_spec = P('dp', 'tp', None, None)
    in_specs = (row_spec, P('dp'), cache_spec, cache_spec, cache_spec, P(None), P(None, None, 'tp', None),
                P(None, 'tp', None), P('tp'), P('tp', None), P('tp', None, None), P(None),
                P(None, 'tp', None, None), P('tp', None, None), P(None), P(None))
    out_specs = (row_spec, cache_spec, cache_spec, cache_spec)

    def local_step(hidden, cache_len, lin_state, k_cache, v_cache, norm_first, w_qkv, w_gate, slopes, out_norm,
                   w_out_lin, norm_second, w_attn, w_out_attn, mix_alpha, mix_beta):
        d = hidden.shape[1]
        cosf, sina, sinb = rope_tables(cache_len)
        state_out, o, gate, h1 = k1(hidden, norm_first.reshape(1, d), w_qkv.reshape(-1, 128),
                                    w_gate.reshape(-1, 128), slopes, lin_state)
        wattn = jnp.transpose(w_attn, (0, 2, 1, 3)).reshape(-1, 128)
        h2, qs, kn, vn = k2(o, gate, h1, out_norm, w_out_lin.reshape(-1, d), norm_second.reshape(1, d), wattn,
                            cosf, sina, sinb, mix_alpha, mix_beta)
        k_out, v_out, attn = k3(k_cache, v_cache, qs, kn, vn, cache_len)
        hidden_out = k4(attn, h2, w_out_attn.reshape(-1, d), mix_alpha, mix_beta)
        return hidden_out, state_out, k_out, v_out

    return jax.shard_map(local_step, mesh=mesh, in_specs=in_specs, out_specs=out_specs, check_vma=False)
```

```python
import functools
import jax
import jax.numpy as jnp
from jax import lax
from jax.experimental import pallas as pl
from jax.experimental.pallas import tpu as pltpu
from jax.sharding import PartitionSpec as P

EPS = 1e-5
ROPE_BASE = 10000000.0
F32 = jnp.float32
BF16 = jnp.bfloat16
MESH = pl.DeviceIdType.MESH
ANY = pl.BlockSpec(memory_space=pl.ANY)
VMEM = pl.BlockSpec(memory_space=pltpu.VMEM)
SMEM = pl.BlockSpec(memory_space=pltpu.SMEM)

DC = 256
RS = 9 * DC + 16
NWB = 4
NSB = 16
LAG = 4


def k1_body(hid_hbm, g1_hbm, wqkv, wgate, slopes_hbm, lin, st_out, o_out, gate_out, h1_out,
            wbuf, gbuf, scr, acc, qq, kk, vv, sbuf, hid, g1, slopes, wsem, rsem, ssem, msem):
    nchunk = hid.shape[1] // DC
    small = [pltpu.make_async_copy(src, dst, msem.at[n])
             for n, (src, dst) in enumerate(((hid_hbm, hid), (g1_hbm, g1), (slopes_hbm, slopes)))]
    for c in small:
        c.start()

    def wcopies(i, slot):
        return (pltpu.make_async_copy(wqkv.at[pl.ds(i * (DC * 24), DC * 24)], wbuf.at[slot], wsem.at[slot, 0]),
                pltpu.make_async_copy(wgate.at[pl.ds(i * (DC * 8), DC * 8)], gbuf.at[slot], wsem.at[slot, 1]))

    def sread(j, slot):
        hp, bb = j // 8, lax.rem(j, 8)
        return pltpu.make_async_copy(lin.at[pl.ds(bb * 8, 8), pl.ds(hp * 2, 2)], sbuf.at[slot], rsem.at[slot])

    def swrite(j, slot):
        hp, bb = j // 8, lax.rem(j, 8)
        return pltpu.make_async_copy(sbuf.at[slot], st_out.at[pl.ds(bb * 8, 8), pl.ds(hp * 2, 2)], ssem.at[slot])

    for i in range(NWB):
        for c in wcopies(i, i):
            c.start()
    for c in small:
        c.wait()
    x = hid[...].astype(F32)
    h1_out[...] = (x * lax.rsqrt(jnp.mean(x * x, axis=-1, keepdims=True) + EPS) * g1[...]).astype(BF16)
    acc[...] = jnp.zeros_like(acc)

    def wstep(i, carry):
        slot = lax.rem(i, NWB)
        for c in wcopies(i, slot):
            c.wait()
        for d2 in range(0, DC, 2):
            t = wbuf[slot, pl.ds(d2 * 24, 48)].astype(F32)
            for u in range(6):
                scr[pl.ds((u % 3) * RS + 9 * (d2 + u // 3), 8, stride=2)] = t[u * 8:(u + 1) * 8]
            t = gbuf[slot, pl.ds(d2 * 8, 16)].astype(F32)
            for u in range(2):
                scr[pl.ds(3 * RS + 9 * (d2 + u), 8, stride=2)] = t[u * 8:(u + 1) * 8]
        hh = h1_out[:, pl.ds(pl.multiple_of(i * DC, DC), DC)]

        def head(m):
            return scr[pl.ds((m // 8) * RS + 2 * (m % 8), DC, stride=9)]

        for n in range(16):
            r = jnp.concatenate([head(2 * n), head(2 * n + 1)], axis=1).astype(BF16)
            acc[:, n * 256:(n + 1) * 256] += jnp.dot(hh, r, preferred_element_type=F32)

        @pl.when(i + NWB < nchunk)
        def _():
            for c in wcopies(i + NWB, slot):
                c.start()

        @pl.when(i < NSB)
        def _():
            sread(i, i).start()
        return carry

    lax.fori_loop(0, nchunk, wstep, 0)

    for hp in range(4):
        def pair(c):
            base = c * 1024 + hp * 256
            return jnp.concatenate([acc[:, base:base + 128], acc[:, base + 128:base + 256]], axis=0)

        def act(c):
            z = pair(c)
            return (z * jax.nn.sigmoid(z)).astype(BF16).astype(F32)
        qq[hp] = act(0)
        kk[hp] = act(1)
        vv[hp] = act(2)
        g = jax.nn.sigmoid(pair(3))
        gate_out[2 * hp] = g[:64]
        gate_out[2 * hp + 1] = g[64:]

    def sstep(j, carry):
        hp, bb = j // 8, lax.rem(j, 8)
        slot = lax.rem(j, NSB)
        sread(j, slot).wait()
        rid = lax.broadcasted_iota(jnp.int32, (16, 128), 0)
        for p in range(2):
            decay = jnp.exp(jnp.full((8, 128), -slopes[hp * 2 + p], F32))[0:1]
            at = pl.ds(p * 64 + bb * 8, 8)
            kq = jnp.concatenate([kk[hp, at], qq[hp, at]], axis=0).T.astype(BF16)
            v16 = jnp.concatenate([vv[hp, at], jnp.zeros((8, 128), F32)], axis=0)
            rows = []
            for i in range(8):
                pick = jnp.concatenate([jnp.where(rid == i, v16, 0.0), jnp.where(rid == 8 + i, 1.0, 0.0)], axis=1)
                both = jnp.dot(kq, pick.astype(BF16), preferred_element_type=F32)
                s_new = decay * sbuf[slot, i, p] + both[:, :128]
                sbuf[slot, i, p] = s_new
                rows.append(jnp.sum(both[:, 128:] * s_new, axis=0, keepdims=True))
            o_out[hp * 2 + p, pl.ds(bb * 8, 8)] = jnp.concatenate(rows, axis=0)
        swrite(j, slot).start()

        @pl.when((j >= LAG) & (j - LAG + NSB < 32))
        def _():
            jj = j - LAG
            ps = lax.rem(jj, NSB)
            swrite(jj, ps).wait()
            sread(jj + NSB, ps).start()
        return carry

    lax.fori_loop(0, 32, sstep, 0)
    for j in range(32 - NSB, 32):
        swrite(j, j % NSB).wait()


def k1(hidden, g1, wqkv, wgate, slopes, lin):
    return pl.pallas_call(
        k1_body,
        out_shape=(jax.ShapeDtypeStruct(lin.shape, F32), jax.ShapeDtypeStruct((8, 64, 128), F32),
                   jax.ShapeDtypeStruct((8, 64, 128), F32), jax.ShapeDtypeStruct(hidden.shape, BF16)),
        in_specs=[ANY] * 6,
        out_specs=(ANY, VMEM, VMEM, VMEM),
        scratch_shapes=[
            pltpu.VMEM((NWB, DC * 24, 128), BF16), pltpu.VMEM((NWB, DC * 8, 128), BF16),
            pltpu.VMEM((4 * RS, 128), F32), pltpu.VMEM((64, 4096), F32),
            pltpu.VMEM((4, 128, 128), F32), pltpu.VMEM((4, 128, 128), F32), pltpu.VMEM((4, 128, 128), F32),
            pltpu.VMEM((NSB, 8, 2, 128, 128), F32),
            pltpu.VMEM(hidden.shape, BF16), pltpu.VMEM(g1.shape, F32), pltpu.SMEM(slopes.shape, F32),
            pltpu.SemaphoreType.DMA((NWB, 2)), pltpu.SemaphoreType.DMA((NSB,)), pltpu.SemaphoreType.DMA((NSB,)),
            pltpu.SemaphoreType.DMA((3,))],
        compiler_params=pltpu.CompilerParams(vmem_limit_bytes=50 * 2 ** 20),
        name='lightning')(hidden, g1, wqkv, wgate, slopes, lin)


NCH = 5
CW = 512
HALF = NCH * CW


def entry_barrier():
    tp = lax.axis_index('tp')
    bar = pltpu.get_barrier_semaphore()
    for peer in peers(tp):
        pl.semaphore_signal(bar, inc=1, device_id={'tp': peer}, device_id_type=MESH)
    pl.semaphore_wait(bar, 3)


def peers(tp):
    core = lax.rem(tp, 2)
    partner = tp + 1 - 2 * core
    across = lax.rem(tp + 2, 4)
    diag = lax.rem(partner + 2, 4)
    return partner, across, diag


def out_weight_copies(w, wo, wosem):
    core = lax.rem(lax.axis_index('tp'), 2)
    out = []
    for s in range(2 * NCH):
        side = core if s % 2 else 1 - core
        col = pl.multiple_of(side * HALF + (s // 2) * CW, CW)
        out.append(pltpu.make_async_copy(w.at[:, pl.ds(col, CW)], wo.at[s], wosem.at[s]))
    return out


def reduce_over_tp(xin, wo, wcopies, full, send_a, recv_a, own, recv_x, sems, between):
    tp = lax.axis_index('tp')
    core = lax.rem(tp, 2)
    partner, across, _ = peers(tp)

    def rcopy(src, dst, k, j, dev):
        return pltpu.make_async_remote_copy(src_ref=src, dst_ref=dst, send_sem=sems.at[k, j],
                                            recv_sem=sems.at[k + 1, j], device_id={'tp': dev}, device_id_type=MESH)
    ca = [rcopy(send_a.at[j], recv_a.at[j], 0, j, partner) for j in range(NCH)]
    cx = [rcopy(own.at[j], recv_x.at[j], 2, j, across) for j in range(NCH)]
    cf = []
    for j in range(NCH):
        col = pl.multiple_of(core * HALF + j * CW, CW)
        cf.append(rcopy(full.at[:, pl.ds(col, CW)], full.at[:, pl.ds(col, CW)], 4, j, partner))

    def combine(j):
        ca[j].wait_recv()
        own[j] = own[j] + recv_a[j]
        cx[j].start()

    for j in range(NCH):
        wcopies[2 * j].wait()
        send_a[j] = jnp.dot(xin[...], wo[2 * j], preferred_element_type=F32)
        ca[j].start()
        wcopies[2 * j + 1].wait()
        own[j] = jnp.dot(xin[...], wo[2 * j + 1], preferred_element_type=F32)
        if j:
            combine(j - 1)
    combine(NCH - 1)
    for j in range(NCH):
        between(j)
        cx[j].wait_recv()
        col = pl.multiple_of(core * HALF + j * CW, CW)
        full[:, pl.ds(col, CW)] = own[j] + recv_x[j]
        cf[j].start()
    for j in range(NCH):
        cf[j].wait_recv()
    for j in range(NCH):
        ca[j].wait_send()
        cx[j].wait_send()
        cf[j].wait_send()


REDUCE_SCRATCH = [
    pltpu.VMEM((64, 2 * HALF), F32), pltpu.VMEM((NCH, 64, CW), F32), pltpu.VMEM((NCH, 64, CW), F32),
    pltpu.VMEM((NCH, 64, CW), F32), pltpu.VMEM((NCH, 64, CW), F32),
    pltpu.VMEM((2 * NCH, 1024, CW), BF16), pltpu.SemaphoreType.DMA((6, NCH)), pltpu.SemaphoreType.DMA((2 * NCH,))]

NAB = 4


def k2_body(o_in, gate_in, h1, onorm, w_out, g2, wattn, cosf, sina, sinb, alpha, beta,
            h2_out, qs, kn, vn,
            full, send_a, recv_a, own, recv_x, wo, sems, wosem,
            xin, ssl, ssr, sssem, abuf, ascr, wd, asem):
    tp = lax.axis_index('tp')
    nchunk = h1.shape[1] // DC
    wcopies = out_weight_copies(w_out, wo, wosem)
    for c in wcopies:
        c.start()

    def acopy(i, slot):
        return pltpu.make_async_copy(wattn.at[pl.ds(i * (DC * 12), DC * 12)], abuf.at[slot], asem.at[slot])
    for i in range(NAB):
        acopy(i, i).start()
    sq = jnp.zeros((64, 128), F32)
    for h in range(8):
        sq = sq + o_in[h] * o_in[h]
    ssl[...] = sq
    entry_barrier()
    copies = [pltpu.make_async_remote_copy(src_ref=ssl, dst_ref=ssr.at[k], send_sem=sssem.at[0, k],
                                           recv_sem=sssem.at[1, k], device_id={'tp': dev}, device_id_type=MESH)
              for k, dev in enumerate(peers(tp))]
    for c in copies:
        c.start()
    for c in copies:
        c.wait_recv()
    total = jnp.sum((ssl[...] + ssr[0]) + (ssr[1] + ssr[2]), axis=-1, keepdims=True)
    inv = lax.rsqrt(total / 4096.0 + EPS)
    for h in range(8):
        xin[:, h * 128:(h + 1) * 128] = (o_in[h] * inv * onorm[h:h + 1] * gate_in[h]).astype(BF16)

    def demix(i, carry):
        slot = lax.rem(i, NAB)
        acopy(i, slot).wait()
        ascr[...] = abuf[slot].astype(F32)
        for j in range(6):
            for kv in range(2):
                wd[j, kv, pl.ds(pl.multiple_of(i * DC, DC), DC)] = ascr[pl.ds(2 * j + kv, DC, stride=12)].astype(BF16)

        @pl.when(i + NAB < nchunk)
        def _():
            acopy(i + NAB, slot).start()
        return carry

    def between(j):
        lax.fori_loop(j * (nchunk // NCH), (j + 1) * (nchunk // NCH), demix, 0)

    reduce_over_tp(xin, wo, wcopies, full, send_a, recv_a, own, recv_x, sems, between)
    for c in copies:
        c.wait_send()
    mid = (alpha[0] * h1[...].astype(F32) + beta[0] * full[...]).astype(BF16).astype(F32)
    h2_out[...] = (mid * lax.rsqrt(jnp.mean(mid * mid, axis=-1, keepdims=True) + EPS) * g2[...]).astype(BF16)
    qs[...] = jnp.zeros_like(qs)

    def turn(z):
        return z * cosf[...] + pltpu.roll(z, 96, 1) * sina[...] + pltpu.roll(z, 32, 1) * sinb[...]

    for j in range(6):
        r = jnp.concatenate([wd[j, 0], wd[j, 1]], axis=1)
        z = jnp.dot(h2_out[...], r, preferred_element_type=F32)
        for kv in range(2):
            zk = z[:, kv * 128:(kv + 1) * 128]
            if j < 4:
                qs[kv, pl.ds(kv * 4 + j, 64, stride=8)] = turn(zk).astype(BF16).astype(F32)
            elif j == 4:
                kn[kv] = turn(zk).astype(BF16).astype(F32)
            else:
                vn[kv] = zk.astype(BF16).astype(F32)


def k2(o, gate, h1, onorm, w_out, g2, wattn, cosf, sina, sinb, alpha, beta):
    return pl.pallas_call(
        k2_body,
        out_shape=(jax.ShapeDtypeStruct(h1.shape, BF16), jax.ShapeDtypeStruct((2, 512, 128), F32),
                   jax.ShapeDtypeStruct((2, 64, 128), F32), jax.ShapeDtypeStruct((2, 64, 128), F32)),
        in_specs=[VMEM, VMEM, VMEM, VMEM, ANY, VMEM, ANY, VMEM, VMEM, VMEM, SMEM, SMEM],
        out_specs=(VMEM, VMEM, VMEM, VMEM),
        scratch_shapes=REDUCE_SCRATCH + [
            pltpu.VMEM((64, 1024), BF16), pltpu.VMEM((64, 128), F32), pltpu.VMEM((3, 64, 128), F32),
            pltpu.SemaphoreType.DMA((2, 3)),
            pltpu.VMEM((NAB, DC * 12, 128), BF16), pltpu.VMEM((DC * 12, 128), F32),
            pltpu.VMEM((6, 2, h1.shape[1], 128), BF16), pltpu.SemaphoreType.DMA((NAB,))],
        compiler_params=pltpu.CompilerParams(vmem_limit_bytes=50 * 2 ** 20, collective_id=0, has_side_effects=True),
        name='mix_first')(o, gate, h1, onorm, w_out, g2, wattn, cosf, sina, sinb, alpha, beta)


NB3 = 8
NS3 = 4


def k3_body(kc, vc, qs, kn, vn, clen, k_out, v_out, attn, kb, vb, sscr, rsem, wsem):
    nstep = kc.shape[0] // NB3

    def reads(i, slot):
        return (pltpu.make_async_copy(kc.at[pl.ds(i * NB3, NB3)], kb.at[slot], rsem.at[slot, 0]),
                pltpu.make_async_copy(vc.at[pl.ds(i * NB3, NB3)], vb.at[slot], rsem.at[slot, 1]))

    def writes(i, slot):
        return (pltpu.make_async_copy(kb.at[slot], k_out.at[pl.ds(i * NB3, NB3)], wsem.at[slot, 0]),
                pltpu.make_async_copy(vb.at[slot], v_out.at[pl.ds(i * NB3, NB3)], wsem.at[slot, 1]))

    for i in range(NS3 - 1):
        for c in reads(i, i):
            c.start()

    def step(i, carry):
        slot = lax.rem(i, NS3)
        for c in reads(i, slot):
            c.wait()
        row_id = lax.broadcasted_iota(jnp.int32, (16, 128), 0)
        for u in range(NB3):
            b = i * NB3 + u
            pos = clen[b]
            base = pl.multiple_of((pos // 16) * 16, 16)
            hit = row_id == pos - base
            for kv in range(2):
                for buf, new in ((kb, kn), (vb, vn)):
                    old = buf[slot, u, kv, pl.ds(base, 16)].astype(F32)
                    row = jnp.broadcast_to(new[kv, pl.ds(b, 1)], (16, 128))
                    buf[slot, u, kv, pl.ds(base, 16)] = jnp.where(hit, row, old).astype(BF16)
        for c in writes(i, slot):
            c.start()

        def score(h, carry):
            for u in range(NB3 // 2):
                w = h * (NB3 // 2) + u
                b = i * NB3 + w
                q = jnp.concatenate([qs[0, pl.ds(b * 8, 8)], qs[1, pl.ds(b * 8, 8)]], axis=1).astype(BF16)
                both = jnp.concatenate([kb[slot, w, 0], kb[slot, w, 1]], axis=1)
                s = lax.dot_general(q, both, (((1,), (1,)), ((), ())), preferred_element_type=F32)
                sscr[w] = s * (128 ** -0.5)
            return carry

        lax.fori_loop(0, 2, score, 0)
        tpos = lax.broadcasted_iota(jnp.int32, (8, 512), 1)
        for w in range(NB3):
            s = jnp.where(tpos <= clen[i * NB3 + w], sscr[w], -jnp.inf)
            e = jnp.exp(s - jnp.max(s, axis=-1, keepdims=True))
            sscr[w] = (e / jnp.sum(e, axis=-1, keepdims=True)).astype(BF16).astype(F32)
        lo = lax.broadcasted_iota(jnp.int32, (8, 128), 0) < 4

        def weigh(h, carry):
            for u in range(NB3 // 2):
                w = h * (NB3 // 2) + u
                b = i * NB3 + w
                both = jnp.concatenate([vb[slot, w, 0], vb[slot, w, 1]], axis=1)
                r = jnp.dot(sscr[w].astype(BF16), both, preferred_element_type=F32)
                attn[pl.ds(b * 8, 8)] = jnp.where(lo, r[:, :128], r[:, 128:]).astype(BF16).astype(F32)
            return carry

        lax.fori_loop(0, 2, weigh, 0)
        nxt = i + NS3 - 1

        @pl.when(nxt < nstep)
        def _():
            ps = lax.rem(nxt, NS3)

            @pl.when(i >= 1)
            def _():
                for c in writes(i - 1, ps):
                    c.wait()
            for c in reads(nxt, ps):
                c.start()
        return carry

    lax.fori_loop(0, nstep, step, 0)
    for i in range(nstep - NS3, nstep):
        for c in writes(i, i % NS3):
            c.wait()


def k3(kc, vc, qs, kn, vn, clen):
    shape = (NS3, NB3) + kc.shape[1:]
    return pl.pallas_call(
        k3_body,
        out_shape=(jax.ShapeDtypeStruct(kc.shape, BF16), jax.ShapeDtypeStruct(vc.shape, BF16),
                   jax.ShapeDtypeStruct((512, 128), F32)),
        in_specs=[ANY, ANY, VMEM, VMEM, VMEM, SMEM],
        out_specs=(ANY, ANY, VMEM),
        scratch_shapes=[pltpu.VMEM(shape, BF16), pltpu.VMEM(shape, BF16), pltpu.VMEM((NB3, 8, 512), F32),
                        pltpu.SemaphoreType.DMA((NS3, 2)), pltpu.SemaphoreType.DMA((NS3, 2))],
        compiler_params=pltpu.CompilerParams(vmem_limit_bytes=50 * 2 ** 20),
        name='attention')(kc, vc, qs, kn, vn, clen)


def k4_body(attn, h2, w_out, alpha, beta, out,
            full, send_a, recv_a, own, recv_x, wo, sems, wosem, xin):
    wcopies = out_weight_copies(w_out, wo, wosem)
    for c in wcopies:
        c.start()
    for r in range(8):
        xin[:, r * 128:(r + 1) * 128] = attn[pl.ds(r, 64, stride=8)].astype(BF16)
    entry_barrier()
    reduce_over_tp(xin, wo, wcopies, full, send_a, recv_a, own, recv_x, sems, lambda j: None)
    out[...] = (alpha[1] * h2[...].astype(F32) + beta[1] * full[...]).astype(BF16)


def k4(attn, h2, w_out, alpha, beta):
    return pl.pallas_call(
        k4_body,
        out_shape=jax.ShapeDtypeStruct(h2.shape, BF16),
        in_specs=[VMEM, VMEM, ANY, SMEM, SMEM],
        out_specs=VMEM,
        scratch_shapes=REDUCE_SCRATCH + [pltpu.VMEM((64, 1024), BF16)],
        compiler_params=pltpu.CompilerParams(vmem_limit_bytes=50 * 2 ** 20, collective_id=1, has_side_effects=True),
        name='mix_second')(attn, h2, w_out, alpha, beta)


def rope_tables(clen):
    inv_freq = ROPE_BASE ** (-2.0 * jnp.arange(32, dtype=F32) / 64)
    ang = clen.astype(F32)[:, None] * inv_freq[None, :]
    cos, sin = jnp.cos(ang), jnp.sin(ang)
    zero = jnp.zeros((clen.shape[0], 32), F32)
    one = jnp.ones((clen.shape[0], 64), F32)
    cosf = jnp.concatenate([cos, cos, one], axis=1)
    sina = jnp.concatenate([-sin, zero, zero, zero], axis=1)
    sinb = jnp.concatenate([zero, sin, zero, zero], axis=1)
    return cosf, sina, sinb


def solution(mesh):
    row_spec = P('dp', None)
    cache_spec = P('dp', 'tp', None, None)
    in_specs = (row_spec, P('dp'), cache_spec, cache_spec, cache_spec, P(None), P(None, None, 'tp', None),
                P(None, 'tp', None), P('tp'), P('tp', None), P('tp', None, None), P(None),
                P(None, 'tp', None, None), P('tp', None, None), P(None), P(None))
    out_specs = (row_spec, cache_spec, cache_spec, cache_spec)

    def local_step(hidden, cache_len, lin_state, k_cache, v_cache, norm_first, w_qkv, w_gate, slopes, out_norm,
                   w_out_lin, norm_second, w_attn, w_out_attn, mix_alpha, mix_beta):
        d = hidden.shape[1]
        cosf, sina, sinb = rope_tables(cache_len)
        state_out, o, gate, h1 = k1(hidden, norm_first.reshape(1, d), w_qkv.reshape(-1, 128),
                                    w_gate.reshape(-1, 128), slopes, lin_state)
        wattn = jnp.transpose(w_attn, (0, 2, 1, 3)).reshape(-1, 128)
        h2, qs, kn, vn = k2(o, gate, h1, out_norm, w_out_lin.reshape(-1, d), norm_second.reshape(1, d), wattn,
                            cosf, sina, sinb, mix_alpha, mix_beta)
        k_out, v_out, attn = k3(k_cache, v_cache, qs, kn, vn, cache_len)
        hidden_out = k4(attn, h2, w_out_attn.reshape(-1, d), mix_alpha, mix_beta)
        return hidden_out, state_out, k_out, v_out

    return jax.shard_map(local_step, mesh=mesh, in_specs=in_specs, out_specs=out_specs, check_vma=False)
```

```python
import math
import jax
import jax.numpy as jnp
from jax import lax
from jax.experimental import pallas as pl
from jax.experimental.pallas import tpu as pltpu
from jax.sharding import PartitionSpec as P

EPS = 1e-5
ROPE_BASE = 10000000.0
F32 = jnp.float32
BF16 = jnp.bfloat16
MESH = pl.DeviceIdType.MESH
ANY = pl.BlockSpec(memory_space=pl.ANY)
HBM = pl.BlockSpec(memory_space=pltpu.HBM)
VMEM = pl.BlockSpec(memory_space=pltpu.VMEM)
SMEM = pl.BlockSpec(memory_space=pltpu.SMEM)

DC = 256
RS = 9 * DC + 16
NWB = 4
NSB = 15
LAG = 4


def k1_body(hid_hbm, g1_hbm, wqkv, wgate, slopes_hbm, lin, st_out, o_out, gate_out, h1_out,
            wbuf, gbuf, scr, acc, qq, kk, vv, sbuf, hid, g1, slopes, wsem, rsem, ssem, msem):
    nchunk = hid.shape[1] // DC
    small = [pltpu.make_async_copy(src, dst, msem.at[n])
             for n, (src, dst) in enumerate(((hid_hbm, hid), (g1_hbm, g1), (slopes_hbm, slopes)))]
    for c in small:
        c.start()

    def wcopies(i, slot):
        return (pltpu.make_async_copy(wqkv.at[pl.ds(i * (DC * 24), DC * 24)], wbuf.at[slot], wsem.at[slot, 0]),
                pltpu.make_async_copy(wgate.at[pl.ds(i * (DC * 8), DC * 8)], gbuf.at[slot], wsem.at[slot, 1]))

    def sread(j, slot):
        hp, bb = j // 8, lax.rem(j, 8)
        return pltpu.make_async_copy(lin.at[pl.ds(bb * 8, 8), pl.ds(hp * 2, 2)], sbuf.at[slot], rsem.at[slot])

    def swrite(j, slot):
        hp, bb = j // 8, lax.rem(j, 8)
        return pltpu.make_async_copy(sbuf.at[slot], st_out.at[pl.ds(bb * 8, 8), pl.ds(hp * 2, 2)], ssem.at[slot])

    for i in range(NWB):
        for c in wcopies(i, i):
            c.start()
    for c in small:
        c.wait()
    x = hid[...].astype(F32)
    h1_out[...] = (x * lax.rsqrt(jnp.mean(x * x, axis=-1, keepdims=True) + EPS) * g1[...]).astype(BF16)
    acc[...] = jnp.zeros_like(acc)

    def wstep(i, carry):
        slot = lax.rem(i, NWB)
        for c in wcopies(i, slot):
            c.wait()
        for d2 in range(0, DC, 2):
            t = wbuf[slot, pl.ds(d2 * 24, 48)].astype(F32)
            for u in range(6):
                scr[pl.ds((u % 3) * RS + 9 * (d2 + u // 3), 8, stride=2)] = t[u * 8:(u + 1) * 8]
            t = gbuf[slot, pl.ds(d2 * 8, 16)].astype(F32)
            for u in range(2):
                scr[pl.ds(3 * RS + 9 * (d2 + u), 8, stride=2)] = t[u * 8:(u + 1) * 8]
        hh = h1_out[:, pl.ds(pl.multiple_of(i * DC, DC), DC)]

        def head(m):
            return scr[pl.ds((m // 8) * RS + 2 * (m % 8), DC, stride=9)]

        for n in range(16):
            r = jnp.concatenate([head(2 * n), head(2 * n + 1)], axis=1).astype(BF16)
            acc[:, n * 256:(n + 1) * 256] += jnp.dot(hh, r, preferred_element_type=F32)

        @pl.when(i + NWB < nchunk)
        def _():
            for c in wcopies(i + NWB, slot):
                c.start()

        @pl.when(i < NSB)
        def _():
            sread(i, i).start()
        return carry

    lax.fori_loop(0, nchunk, wstep, 0)

    for hp in range(4):
        def pair(c):
            base = c * 1024 + hp * 256
            return jnp.concatenate([acc[:, base:base + 128], acc[:, base + 128:base + 256]], axis=0)

        def act(c):
            z = pair(c)
            return (z * jax.nn.sigmoid(z)).astype(BF16).astype(F32)
        qq[hp] = act(0)
        kk[hp] = act(1)
        vv[hp] = act(2)
        g = jax.nn.sigmoid(pair(3))
        gate_out[2 * hp] = g[:64]
        gate_out[2 * hp + 1] = g[64:]

    def sstep(j, carry):
        hp, bb = j // 8, lax.rem(j, 8)
        slot = lax.rem(j, NSB)
        sread(j, slot).wait()
        rid = lax.broadcasted_iota(jnp.int32, (16, 128), 0)
        for p in range(2):
            decay = jnp.exp(jnp.full((8, 128), -slopes[hp * 2 + p], F32))[0:1]
            at = pl.ds(p * 64 + bb * 8, 8)
            kq = jnp.concatenate([kk[hp, at], qq[hp, at]], axis=0).T.astype(BF16)
            v16 = jnp.concatenate([vv[hp, at], jnp.zeros((8, 128), F32)], axis=0)
            rows = []
            for i in range(8):
                pick = jnp.concatenate([jnp.where(rid == i, v16, 0.0), jnp.where(rid == 8 + i, 1.0, 0.0)], axis=1)
                both = jnp.dot(kq, pick.astype(BF16), preferred_element_type=F32)
                s_new = decay * sbuf[slot, i, p] + both[:, :128]
                sbuf[slot, i, p] = s_new
                rows.append(jnp.sum(both[:, 128:] * s_new, axis=0, keepdims=True))
            o_out[hp * 2 + p, pl.ds(bb * 8, 8)] = jnp.concatenate(rows, axis=0)
        swrite(j, slot).start()

        @pl.when((j >= LAG) & (j - LAG + NSB < 32))
        def _():
            jj = j - LAG
            ps = lax.rem(jj, NSB)
            swrite(jj, ps).wait()
            sread(jj + NSB, ps).start()
        return carry

    lax.fori_loop(0, 32, sstep, 0)
    for j in range(32 - NSB, 32):
        swrite(j, j % NSB).wait()


def k1(hidden, g1, wqkv, wgate, slopes, lin):
    return pl.pallas_call(
        k1_body,
        out_shape=(jax.ShapeDtypeStruct(lin.shape, F32), jax.ShapeDtypeStruct((8, 64, 128), F32),
                   jax.ShapeDtypeStruct((8, 64, 128), F32), jax.ShapeDtypeStruct(hidden.shape, BF16)),
        in_specs=[HBM] * 6,
        out_specs=(ANY, VMEM, VMEM, VMEM),
        scratch_shapes=[
            pltpu.VMEM((NWB, DC * 24, 128), BF16), pltpu.VMEM((NWB, DC * 8, 128), BF16),
            pltpu.VMEM((4 * RS, 128), F32), pltpu.VMEM((64, 4096), F32),
            pltpu.VMEM((4, 128, 128), F32), pltpu.VMEM((4, 128, 128), F32), pltpu.VMEM((4, 128, 128), F32),
            pltpu.VMEM((NSB, 8, 2, 128, 128), F32),
            pltpu.VMEM(hidden.shape, BF16), pltpu.VMEM(g1.shape, F32), pltpu.SMEM(slopes.shape, F32),
            pltpu.SemaphoreType.DMA((NWB, 2)), pltpu.SemaphoreType.DMA((NSB,)), pltpu.SemaphoreType.DMA((NSB,)),
            pltpu.SemaphoreType.DMA((3,))],
        compiler_params=pltpu.CompilerParams(vmem_limit_bytes=34 * 2 ** 20),
        cost_estimate=pl.CostEstimate(flops=int(5e9), bytes_accessed=int(1.1e8), transcendentals=0),
        name='lightning')(hidden, g1, wqkv, wgate, slopes, lin)


NCH = 5
CW = 512
HALF = NCH * CW


def entry_barrier():
    tp = lax.axis_index('tp')
    bar = pltpu.get_barrier_semaphore()
    for peer in peers(tp):
        pl.semaphore_signal(bar, inc=1, device_id={'tp': peer}, device_id_type=MESH)
    pl.semaphore_wait(bar, 3)


def peers(tp):
    core = lax.rem(tp, 2)
    partner = tp + 1 - 2 * core
    across = lax.rem(tp + 2, 4)
    diag = lax.rem(partner + 2, 4)
    return partner, across, diag


def reduce_over_tp(xin, w, full, send_a, recv_a, own, recv_x, sems, between):
    tp = lax.axis_index('tp')
    core = lax.rem(tp, 2)
    partner, across, _ = peers(tp)

    def rcopy(src, dst, k, j, dev):
        return pltpu.make_async_remote_copy(src_ref=src, dst_ref=dst, send_sem=sems.at[k, j],
                                            recv_sem=sems.at[k + 1, j], device_id={'tp': dev}, device_id_type=MESH)
    ca = [rcopy(send_a.at[j], recv_a.at[j], 0, j, partner) for j in range(NCH)]
    cx = [rcopy(own.at[j], recv_x.at[j], 2, j, across) for j in range(NCH)]
    cf = []
    for j in range(NCH):
        col = pl.multiple_of(core * HALF + j * CW, CW)
        cf.append(rcopy(full.at[:, pl.ds(col, CW)], full.at[:, pl.ds(col, CW)], 4, j, partner))

    def combine(j):
        ca[j].wait_recv()
        own[j] = own[j] + recv_a[j]
        cx[j].start()

    for j in range(NCH):
        far = pl.multiple_of((1 - core) * HALF + j * CW, CW)
        send_a[j] = jnp.dot(xin[...], w[:, pl.ds(far, CW)], preferred_element_type=F32)
        ca[j].start()
        near = pl.multiple_of(core * HALF + j * CW, CW)
        own[j] = jnp.dot(xin[...], w[:, pl.ds(near, CW)], preferred_element_type=F32)
        if j:
            combine(j - 1)
    combine(NCH - 1)
    for j in range(NCH):
        between(j)
        cx[j].wait_recv()
        col = pl.multiple_of(core * HALF + j * CW, CW)
        full[:, pl.ds(col, CW)] = own[j] + recv_x[j]
        cf[j].start()
    for j in range(NCH):
        cf[j].wait_recv()
    for j in range(NCH):
        ca[j].wait_send()
        cx[j].wait_send()
        cf[j].wait_send()


REDUCE_SCRATCH = [
    pltpu.VMEM((64, 2 * HALF), F32), pltpu.VMEM((NCH, 64, CW), F32), pltpu.VMEM((NCH, 64, CW), F32),
    pltpu.VMEM((NCH, 64, CW), F32), pltpu.VMEM((NCH, 64, CW), F32),
    pltpu.SemaphoreType.DMA((6, NCH))]

NAB = 4
DA = 128


def k2_body(o_in, gate_in, h1, onorm, w_out, g2, wattn, clen, alpha, beta,
            h2_out, qs, kn, vn,
            full, send_a, recv_a, own, recv_x, sems,
            xin, ssl, ssr, sssem, abuf, ascr, wd, asem, cosf, sina, sinb):
    tp = lax.axis_index('tp')
    nchunk = h1.shape[1] // DA

    def acopy(i, slot):
        return pltpu.make_async_copy(wattn.at[pl.ds(i * (DA * 12), DA * 12)], abuf.at[slot], asem.at[slot])
    for i in range(NAB):
        acopy(i, i).start()
    sq = jnp.zeros((64, 128), F32)
    for h in range(8):
        sq = sq + o_in[h] * o_in[h]
    ssl[...] = sq
    entry_barrier()
    copies = [pltpu.make_async_remote_copy(src_ref=ssl, dst_ref=ssr.at[k], send_sem=sssem.at[0, k],
                                           recv_sem=sssem.at[1, k], device_id={'tp': dev}, device_id_type=MESH)
              for k, dev in enumerate(peers(tp))]
    for c in copies:
        c.start()
    def spread(b, carry):
        cosf[pl.ds(b, 1)] = jnp.full((1, 128), clen[b].astype(F32), F32)
        return carry

    lax.fori_loop(0, 64, spread, 0)
    lane = lax.broadcasted_iota(jnp.int32, (64, 128), 1)
    power = (lane & 31).astype(F32) * (-2.0 / 64)
    angle = cosf[...] * jnp.exp(power * math.log(ROPE_BASE))
    sine = jnp.sin(angle)
    cosf[...] = jnp.where(lane < 64, jnp.cos(angle), 1.0)
    sina[...] = jnp.where(lane < 32, -sine, 0.0)
    sinb[...] = jnp.where((lane >= 32) & (lane < 64), sine, 0.0)
    for c in copies:
        c.wait_recv()
    total = jnp.sum((ssl[...] + ssr[0]) + (ssr[1] + ssr[2]), axis=-1, keepdims=True)
    inv = lax.rsqrt(total / 4096.0 + EPS)
    for h in range(8):
        xin[:, h * 128:(h + 1) * 128] = (o_in[h] * inv * onorm[h:h + 1] * gate_in[h]).astype(BF16)

    def demix(i, carry):
        slot = lax.rem(i, NAB)
        acopy(i, slot).wait()
        ascr[...] = abuf[slot].astype(F32)
        for j in range(6):
            for kv in range(2):
                wd[j, kv, pl.ds(pl.multiple_of(i * DA, DA), DA)] = ascr[pl.ds(2 * j + kv, DA, stride=12)].astype(BF16)

        @pl.when(i + NAB < nchunk)
        def _():
            acopy(i + NAB, slot).start()
        return carry

    def between(j):
        lax.fori_loop(j * (nchunk // NCH), (j + 1) * (nchunk // NCH), demix, 0)

    reduce_over_tp(xin, w_out, full, send_a, recv_a, own, recv_x, sems, between)
    for c in copies:
        c.wait_send()
    mid = (alpha[0] * h1[...].astype(F32) + beta[0] * full[...]).astype(BF16).astype(F32)
    h2_out[...] = (mid * lax.rsqrt(jnp.mean(mid * mid, axis=-1, keepdims=True) + EPS) * g2[...]).astype(BF16)
    qs[...] = jnp.zeros_like(qs)

    def turn(z):
        return z * cosf[...] + pltpu.roll(z, 96, 1) * sina[...] + pltpu.roll(z, 32, 1) * sinb[...]

    for j in range(6):
        r = jnp.concatenate([wd[j, 0], wd[j, 1]], axis=1)
        z = jnp.dot(h2_out[...], r, preferred_element_type=F32)
        for kv in range(2):
            zk = z[:, kv * 128:(kv + 1) * 128]
            if j < 4:
                qs[kv, pl.ds(kv * 4 + j, 64, stride=8)] = turn(zk).astype(BF16).astype(F32)
            elif j == 4:
                kn[kv] = turn(zk).astype(BF16).astype(F32)
            else:
                vn[kv] = zk.astype(BF16).astype(F32)


def k2(o, gate, h1, onorm, w_out, g2, wattn, clen, alpha, beta):
    return pl.pallas_call(
        k2_body,
        out_shape=(jax.ShapeDtypeStruct(h1.shape, BF16), jax.ShapeDtypeStruct((2, 512, 128), F32),
                   jax.ShapeDtypeStruct((2, 64, 128), F32), jax.ShapeDtypeStruct((2, 64, 128), F32)),
        in_specs=[VMEM, VMEM, VMEM, VMEM, VMEM, VMEM, HBM, SMEM, SMEM, SMEM],
        out_specs=(VMEM, VMEM, VMEM, VMEM),
        scratch_shapes=REDUCE_SCRATCH + [
            pltpu.VMEM((64, 1024), BF16), pltpu.VMEM((64, 128), F32), pltpu.VMEM((3, 64, 128), F32),
            pltpu.SemaphoreType.DMA((2, 3)),
            pltpu.VMEM((NAB, DA * 12, 128), BF16), pltpu.VMEM((DA * 12, 128), F32),
            pltpu.VMEM((6, 2, h1.shape[1], 128), BF16), pltpu.SemaphoreType.DMA((NAB,)),
            pltpu.VMEM((64, 128), F32), pltpu.VMEM((64, 128), F32), pltpu.VMEM((64, 128), F32)],
        compiler_params=pltpu.CompilerParams(vmem_limit_bytes=24 * 2 ** 20, collective_id=0, has_side_effects=True),
        cost_estimate=pl.CostEstimate(flops=int(6e10), bytes_accessed=int(2e7), transcendentals=0),
        name='mix_first')(o, gate, h1, onorm, w_out, g2, wattn, clen, alpha, beta)


NB3 = 8
NS3 = 4


def k3_body(kc, vc, qs, kn, vn, clen, k_out, v_out, attn, kb, vb, sscr, rsem, wsem):
    nstep = kc.shape[0] // NB3

    def reads(i, slot):
        return (pltpu.make_async_copy(vc.at[pl.ds(i * NB3, NB3)], vb.at[slot], rsem.at[slot, 1]),)

    def writes(i, slot):
        return (pltpu.make_async_copy(kb.at[slot], k_out.at[pl.ds(i * NB3, NB3)], wsem.at[slot, 0]),
                pltpu.make_async_copy(vb.at[slot], v_out.at[pl.ds(i * NB3, NB3)], wsem.at[slot, 1]))

    for i in range(NS3 - 1):
        for c in reads(i, i):
            c.start()

    def step(i, carry):
        slot = lax.rem(i, NS3)
        for c in reads(i, slot):
            c.wait()
        kb[slot] = kc[pl.ds(i * NB3, NB3)]
        row_id = lax.broadcasted_iota(jnp.int32, (16, 128), 0)
        for u in range(NB3):
            b = i * NB3 + u
            pos = clen[b]
            base = pl.multiple_of((pos // 16) * 16, 16)
            hit = row_id == pos - base
            for kv in range(2):
                for buf, new in ((kb, kn), (vb, vn)):
                    old = buf[slot, u, kv, pl.ds(base, 16)].astype(F32)
                    row = jnp.broadcast_to(new[kv, pl.ds(b, 1)], (16, 128))
                    buf[slot, u, kv, pl.ds(base, 16)] = jnp.where(hit, row, old).astype(BF16)
        for c in writes(i, slot):
            c.start()

        def score(h, carry):
            for u in range(NB3 // 2):
                w = h * (NB3 // 2) + u
                b = i * NB3 + w
                q = jnp.concatenate([qs[0, pl.ds(b * 8, 8)], qs[1, pl.ds(b * 8, 8)]], axis=1).astype(BF16)
                both = jnp.concatenate([kb[slot, w, 0], kb[slot, w, 1]], axis=1)
                s = lax.dot_general(q, both, (((1,), (1,)), ((), ())), preferred_element_type=F32)
                sscr[w] = s * (128 ** -0.5)
            return carry

        lax.fori_loop(0, 2, score, 0)
        tpos = lax.broadcasted_iota(jnp.int32, (8, 512), 1)
        for w in range(NB3):
            s = jnp.where(tpos <= clen[i * NB3 + w], sscr[w], -jnp.inf)
            e = jnp.exp(s - jnp.max(s, axis=-1, keepdims=True))
            sscr[w] = (e / jnp.sum(e, axis=-1, keepdims=True)).astype(BF16).astype(F32)
        lo = lax.broadcasted_iota(jnp.int32, (8, 128), 0) < 4

        def weigh(h, carry):
            for u in range(NB3 // 2):
                w = h * (NB3 // 2) + u
                b = i * NB3 + w
                both = jnp.concatenate([vb[slot, w, 0], vb[slot, w, 1]], axis=1)
                r = jnp.dot(sscr[w].astype(BF16), both, preferred_element_type=F32)
                attn[pl.ds(b * 8, 8)] = jnp.where(lo, r[:, :128], r[:, 128:]).astype(BF16).astype(F32)
            return carry

        lax.fori_loop(0, 2, weigh, 0)
        nxt = i + NS3 - 1

        @pl.when(nxt < nstep)
        def _():
            ps = lax.rem(nxt, NS3)

            @pl.when(i >= 1)
            def _():
                for c in writes(i - 1, ps):
                    c.wait()
            for c in reads(nxt, ps):
                c.start()
        return carry

    lax.fori_loop(0, nstep, step, 0)
    for i in range(nstep - NS3, nstep):
        for c in writes(i, i % NS3):
            c.wait()


def k3(kc, vc, qs, kn, vn, clen):
    shape = (NS3, NB3) + kc.shape[1:]
    return pl.pallas_call(
        k3_body,
        out_shape=(jax.ShapeDtypeStruct(kc.shape, BF16), jax.ShapeDtypeStruct(vc.shape, BF16),
                   jax.ShapeDtypeStruct((512, 128), F32)),
        in_specs=[VMEM, HBM, VMEM, VMEM, VMEM, SMEM],
        out_specs=(ANY, ANY, VMEM),
        scratch_shapes=[pltpu.VMEM(shape, BF16), pltpu.VMEM(shape, BF16), pltpu.VMEM((NB3, 8, 512), F32),
                        pltpu.SemaphoreType.DMA((NS3, 2)), pltpu.SemaphoreType.DMA((NS3, 2))],
        compiler_params=pltpu.CompilerParams(vmem_limit_bytes=20 * 2 ** 20),
        cost_estimate=pl.CostEstimate(flops=int(1e9), bytes_accessed=int(6e7), transcendentals=0),
        name='attention')(kc, vc, qs, kn, vn, clen)


def k4_body(attn, h2, w_out, alpha, beta, out,
            full, send_a, recv_a, own, recv_x, sems, xin):
    for r in range(8):
        xin[:, r * 128:(r + 1) * 128] = attn[pl.ds(r, 64, stride=8)].astype(BF16)
    entry_barrier()
    reduce_over_tp(xin, w_out, full, send_a, recv_a, own, recv_x, sems, lambda j: None)
    out[...] = (alpha[1] * h2[...].astype(F32) + beta[1] * full[...]).astype(BF16)


def k4(attn, h2, w_out, alpha, beta):
    return pl.pallas_call(
        k4_body,
        out_shape=jax.ShapeDtypeStruct(h2.shape, BF16),
        in_specs=[VMEM, VMEM, VMEM, SMEM, SMEM],
        out_specs=VMEM,
        scratch_shapes=REDUCE_SCRATCH + [pltpu.VMEM((64, 1024), BF16)],
        compiler_params=pltpu.CompilerParams(vmem_limit_bytes=11 * 2 ** 20, collective_id=1, has_side_effects=True),
        cost_estimate=pl.CostEstimate(flops=int(2e10), bytes_accessed=int(2e6), transcendentals=0),
        name='mix_second')(attn, h2, w_out, alpha, beta)


def solution(mesh):
    row_spec = P('dp', None)
    cache_spec = P('dp', 'tp', None, None)
    in_specs = (row_spec, P('dp'), cache_spec, cache_spec, cache_spec, P(None), P(None, None, 'tp', None),
                P(None, 'tp', None), P('tp'), P('tp', None), P('tp', None, None), P(None),
                P(None, 'tp', None, None), P('tp', None, None), P(None), P(None))
    out_specs = (row_spec, cache_spec, cache_spec, cache_spec)

    def local_step(hidden, cache_len, lin_state, k_cache, v_cache, norm_first, w_qkv, w_gate, slopes, out_norm,
                   w_out_lin, norm_second, w_attn, w_out_attn, mix_alpha, mix_beta):
        d = hidden.shape[1]

        def pin(x):
            return pltpu.with_memory_space_constraint(x, pltpu.HBM)
        state_out, o, gate, h1 = k1(pin(hidden), pin(norm_first.reshape(1, d)), pin(w_qkv.reshape(-1, 128)),
                                    pin(w_gate.reshape(-1, 128)), pin(slopes), pin(lin_state))
        wattn = pin(jnp.transpose(w_attn, (0, 2, 1, 3)).reshape(-1, 128))
        h2, qs, kn, vn = k2(o, gate, h1, out_norm, w_out_lin.reshape(-1, d), norm_second.reshape(1, d), wattn,
                            cache_len, mix_alpha, mix_beta)
        k_out, v_out, attn = k3(k_cache, pin(v_cache), qs, kn, vn, cache_len)
        hidden_out = k4(attn, h2, w_out_attn.reshape(-1, d), mix_alpha, mix_beta)
        return hidden_out, state_out, k_out, v_out

    return jax.shard_map(local_step, mesh=mesh, in_specs=in_specs, out_specs=out_specs, check_vma=False)
```

```python
import math
import jax
import jax.numpy as jnp
from jax import lax
from jax.experimental import pallas as pl
from jax.experimental.pallas import tpu as pltpu
from jax.sharding import PartitionSpec as P

EPS = 1e-5
ROPE_BASE = 10000000.0
F32 = jnp.float32
BF16 = jnp.bfloat16
MESH = pl.DeviceIdType.MESH
ANY = pl.BlockSpec(memory_space=pl.ANY)
HBM = pl.BlockSpec(memory_space=pltpu.HBM)
VMEM = pl.BlockSpec(memory_space=pltpu.VMEM)
SMEM = pl.BlockSpec(memory_space=pltpu.SMEM)

DC = 256
RS = 9 * DC + 16
NWB = 4
NSB = 15
LAG = 4


def k1_body(hid_hbm, g1_hbm, wqkv, wgate, slopes_hbm, lin, st_out, o_out, gate_out, h1_out,
            wbuf, gbuf, scr, acc, qq, kk, vv, sbuf, hid, g1, slopes, wsem, rsem, ssem, msem):
    nchunk = hid.shape[1] // DC
    small = [pltpu.make_async_copy(src, dst, msem.at[n])
             for n, (src, dst) in enumerate(((hid_hbm, hid), (g1_hbm, g1), (slopes_hbm, slopes)))]
    for c in small:
        c.start()

    def wcopies(i, slot):
        return (pltpu.make_async_copy(wqkv.at[pl.ds(i * (DC * 24), DC * 24)], wbuf.at[slot], wsem.at[slot, 0]),
                pltpu.make_async_copy(wgate.at[pl.ds(i * (DC * 8), DC * 8)], gbuf.at[slot], wsem.at[slot, 1]))

    def sread(j, slot):
        hp, bb = j // 8, lax.rem(j, 8)
        return pltpu.make_async_copy(lin.at[pl.ds(bb * 8, 8), pl.ds(hp * 2, 2)], sbuf.at[slot], rsem.at[slot])

    def swrite(j, slot):
        hp, bb = j // 8, lax.rem(j, 8)
        return pltpu.make_async_copy(sbuf.at[slot], st_out.at[pl.ds(bb * 8, 8), pl.ds(hp * 2, 2)], ssem.at[slot])

    for i in range(NWB):
        for c in wcopies(i, i):
            c.start()
    for c in small:
        c.wait()
    x = hid[...].astype(F32)
    h1_out[...] = (x * lax.rsqrt(jnp.mean(x * x, axis=-1, keepdims=True) + EPS) * g1[...]).astype(BF16)
    acc[...] = jnp.zeros_like(acc)

    def wstep(i, carry):
        slot = lax.rem(i, NWB)
        for c in wcopies(i, slot):
            c.wait()
        for d2 in range(0, DC, 2):
            t = wbuf[slot, pl.ds(d2 * 24, 48)].astype(F32)
            for u in range(6):
                scr[pl.ds((u % 3) * RS + 9 * (d2 + u // 3), 8, stride=2)] = t[u * 8:(u + 1) * 8]
            t = gbuf[slot, pl.ds(d2 * 8, 16)].astype(F32)
            for u in range(2):
                scr[pl.ds(3 * RS + 9 * (d2 + u), 8, stride=2)] = t[u * 8:(u + 1) * 8]
        hh = h1_out[:, pl.ds(pl.multiple_of(i * DC, DC), DC)]

        def head(m):
            return scr[pl.ds((m // 8) * RS + 2 * (m % 8), DC, stride=9)]

        for n in range(16):
            r = jnp.concatenate([head(2 * n), head(2 * n + 1)], axis=1).astype(BF16)
            acc[:, n * 256:(n + 1) * 256] += jnp.dot(hh, r, preferred_element_type=F32)

        @pl.when(i + NWB < nchunk)
        def _():
            for c in wcopies(i + NWB, slot):
                c.start()

        @pl.when(i < NSB)
        def _():
            sread(i, i).start()
        return carry

    lax.fori_loop(0, nchunk, wstep, 0)

    for hp in range(4):
        def pair(c):
            base = c * 1024 + hp * 256
            return jnp.concatenate([acc[:, base:base + 128], acc[:, base + 128:base + 256]], axis=0)

        def act(c):
            z = pair(c)
            return (z * jax.nn.sigmoid(z)).astype(BF16).astype(F32)
        qq[hp] = act(0)
        kk[hp] = act(1)
        vv[hp] = act(2)
        g = jax.nn.sigmoid(pair(3))
        gate_out[2 * hp] = g[:64]
        gate_out[2 * hp + 1] = g[64:]

    def sstep(j, carry):
        hp, bb = j // 8, lax.rem(j, 8)
        slot = lax.rem(j, NSB)
        sread(j, slot).wait()
        rid = lax.broadcasted_iota(jnp.int32, (16, 128), 0)
        for p in range(2):
            decay = jnp.exp(jnp.full((8, 128), -slopes[hp * 2 + p], F32))[0:1]
            at = pl.ds(p * 64 + bb * 8, 8)
            kq = jnp.concatenate([kk[hp, at], qq[hp, at]], axis=0).T.astype(BF16)
            v16 = jnp.concatenate([vv[hp, at], jnp.zeros((8, 128), F32)], axis=0)
            rows = []
            for i in range(8):
                pick = jnp.concatenate([jnp.where(rid == i, v16, 0.0), jnp.where(rid == 8 + i, 1.0, 0.0)], axis=1)
                both = jnp.dot(kq, pick.astype(BF16), preferred_element_type=F32)
                s_new = decay * sbuf[slot, i, p] + both[:, :128]
                sbuf[slot, i, p] = s_new
                rows.append(jnp.sum(both[:, 128:] * s_new, axis=0, keepdims=True))
            o_out[hp * 2 + p, pl.ds(bb * 8, 8)] = jnp.concatenate(rows, axis=0)
        swrite(j, slot).start()

        @pl.when((j >= LAG) & (j - LAG + NSB < 32))
        def _():
            jj = j - LAG
            ps = lax.rem(jj, NSB)
            swrite(jj, ps).wait()
            sread(jj + NSB, ps).start()
        return carry

    lax.fori_loop(0, 32, sstep, 0)
    for j in range(32 - NSB, 32):
        swrite(j, j % NSB).wait()


def k1(hidden, g1, wqkv, wgate, slopes, lin):
    return pl.pallas_call(
        k1_body,
        out_shape=(jax.ShapeDtypeStruct(lin.shape, F32), jax.ShapeDtypeStruct((8, 64, 128), F32),
                   jax.ShapeDtypeStruct((8, 64, 128), F32), jax.ShapeDtypeStruct(hidden.shape, BF16)),
        in_specs=[HBM] * 6,
        out_specs=(ANY, VMEM, VMEM, VMEM),
        scratch_shapes=[
            pltpu.VMEM((NWB, DC * 24, 128), BF16), pltpu.VMEM((NWB, DC * 8, 128), BF16),
            pltpu.VMEM((4 * RS, 128), F32), pltpu.VMEM((64, 4096), F32),
            pltpu.VMEM((4, 128, 128), F32), pltpu.VMEM((4, 128, 128), F32), pltpu.VMEM((4, 128, 128), F32),
            pltpu.VMEM((NSB, 8, 2, 128, 128), F32),
            pltpu.VMEM(hidden.shape, BF16), pltpu.VMEM(g1.shape, F32), pltpu.SMEM(slopes.shape, F32),
            pltpu.SemaphoreType.DMA((NWB, 2)), pltpu.SemaphoreType.DMA((NSB,)), pltpu.SemaphoreType.DMA((NSB,)),
            pltpu.SemaphoreType.DMA((3,))],
        compiler_params=pltpu.CompilerParams(vmem_limit_bytes=34 * 2 ** 20),
        cost_estimate=pl.CostEstimate(flops=int(1e12), bytes_accessed=int(1.1e8), transcendentals=0),
        name='lightning')(hidden, g1, wqkv, wgate, slopes, lin)


NCH = 5
CW = 512
HALF = NCH * CW


def entry_barrier():
    tp = lax.axis_index('tp')
    bar = pltpu.get_barrier_semaphore()
    for peer in peers(tp):
        pl.semaphore_signal(bar, inc=1, device_id={'tp': peer}, device_id_type=MESH)
    pl.semaphore_wait(bar, 3)


def peers(tp):
    core = lax.rem(tp, 2)
    partner = tp + 1 - 2 * core
    across = lax.rem(tp + 2, 4)
    diag = lax.rem(partner + 2, 4)
    return partner, across, diag


def out_weight_copies(w, wo, wosem):
    core = lax.rem(lax.axis_index('tp'), 2)
    out = []
    for s in range(2 * NCH):
        side = core if s % 2 else 1 - core
        col = pl.multiple_of(side * HALF + (s // 2) * CW, CW)
        out.append(pltpu.make_async_copy(w.at[:, pl.ds(col, CW)], wo.at[s], wosem.at[s]))
    return out


def reduce_over_tp(xin, wo, wcopies, full, send_a, recv_a, own, recv_x, sems, between):
    tp = lax.axis_index('tp')
    core = lax.rem(tp, 2)
    partner, across, _ = peers(tp)

    def rcopy(src, dst, k, j, dev):
        return pltpu.make_async_remote_copy(src_ref=src, dst_ref=dst, send_sem=sems.at[k, j],
                                            recv_sem=sems.at[k + 1, j], device_id={'tp': dev}, device_id_type=MESH)
    ca = [rcopy(send_a.at[j], recv_a.at[j], 0, j, partner) for j in range(NCH)]
    cx = [rcopy(own.at[j], recv_x.at[j], 2, j, across) for j in range(NCH)]
    cf = []
    for j in range(NCH):
        col = pl.multiple_of(core * HALF + j * CW, CW)
        cf.append(rcopy(full.at[:, pl.ds(col, CW)], full.at[:, pl.ds(col, CW)], 4, j, partner))

    def combine(j):
        ca[j].wait_recv()
        own[j] = own[j] + recv_a[j]
        cx[j].start()

    for j in range(NCH):
        wcopies[2 * j].wait()
        send_a[j] = jnp.dot(xin[...], wo[2 * j], preferred_element_type=F32)
        ca[j].start()
        wcopies[2 * j + 1].wait()
        own[j] = jnp.dot(xin[...], wo[2 * j + 1], preferred_element_type=F32)
        if j:
            combine(j - 1)
    combine(NCH - 1)
    for j in range(NCH):
        between(j)
        cx[j].wait_recv()
        col = pl.multiple_of(core * HALF + j * CW, CW)
        full[:, pl.ds(col, CW)] = own[j] + recv_x[j]
        cf[j].start()
    for j in range(NCH):
        cf[j].wait_recv()
    for j in range(NCH):
        ca[j].wait_send()
        cx[j].wait_send()
        cf[j].wait_send()


REDUCE_SCRATCH = [
    pltpu.VMEM((64, 2 * HALF), F32), pltpu.VMEM((NCH, 64, CW), F32), pltpu.VMEM((NCH, 64, CW), F32),
    pltpu.VMEM((NCH, 64, CW), F32), pltpu.VMEM((NCH, 64, CW), F32),
    pltpu.VMEM((2 * NCH, 1024, CW), BF16), pltpu.SemaphoreType.DMA((6, NCH)), pltpu.SemaphoreType.DMA((2 * NCH,))]

NAB = 8
DA = 128


def k2_body(o_in, gate_in, h1, onorm, w_out, g2, wattn, clen, alpha, beta,
            h2_out, qs, kn, vn,
            full, send_a, recv_a, own, recv_x, wo, sems, wosem,
            xin, ssl, ssr, sssem, abuf, ascr, wd, asem, cosf, sina, sinb):
    tp = lax.axis_index('tp')
    nchunk = h1.shape[1] // DA
    wcopies = out_weight_copies(w_out, wo, wosem)
    for c in wcopies:
        c.start()

    def acopy(i, slot):
        return pltpu.make_async_copy(wattn.at[pl.ds(i * (DA * 12), DA * 12)], abuf.at[slot], asem.at[slot])
    for i in range(NAB):
        acopy(i, i).start()
    sq = jnp.zeros((64, 128), F32)
    for h in range(8):
        sq = sq + o_in[h] * o_in[h]
    ssl[...] = sq
    entry_barrier()
    copies = [pltpu.make_async_remote_copy(src_ref=ssl, dst_ref=ssr.at[k], send_sem=sssem.at[0, k],
                                           recv_sem=sssem.at[1, k], device_id={'tp': dev}, device_id_type=MESH)
              for k, dev in enumerate(peers(tp))]
    for c in copies:
        c.start()
    def spread(b, carry):
        cosf[pl.ds(b, 1)] = jnp.full((1, 128), clen[b].astype(F32), F32)
        return carry

    lax.fori_loop(0, 64, spread, 0)
    lane = lax.broadcasted_iota(jnp.int32, (64, 128), 1)
    power = (lane & 31).astype(F32) * (-2.0 / 64)
    angle = cosf[...] * jnp.exp(power * math.log(ROPE_BASE))
    sine = jnp.sin(angle)
    cosf[...] = jnp.where(lane < 64, jnp.cos(angle), 1.0)
    sina[...] = jnp.where(lane < 32, -sine, 0.0)
    sinb[...] = jnp.where((lane >= 32) & (lane < 64), sine, 0.0)
    for c in copies:
        c.wait_recv()
    total = jnp.sum((ssl[...] + ssr[0]) + (ssr[1] + ssr[2]), axis=-1, keepdims=True)
    inv = lax.rsqrt(total / 4096.0 + EPS)
    for h in range(8):
        xin[:, h * 128:(h + 1) * 128] = (o_in[h] * inv * onorm[h:h + 1] * gate_in[h]).astype(BF16)

    def demix(i, carry):
        slot = lax.rem(i, NAB)
        acopy(i, slot).wait()
        ascr[...] = abuf[slot].astype(F32)
        for j in range(6):
            for kv in range(2):
                wd[j, kv, pl.ds(pl.multiple_of(i * DA, DA), DA)] = ascr[pl.ds(2 * j + kv, DA, stride=12)].astype(BF16)

        @pl.when(i + NAB < nchunk)
        def _():
            acopy(i + NAB, slot).start()
        return carry

    def between(j):
        lax.fori_loop(j * (nchunk // NCH), (j + 1) * (nchunk // NCH), demix, 0)

    reduce_over_tp(xin, wo, wcopies, full, send_a, recv_a, own, recv_x, sems, between)
    for c in copies:
        c.wait_send()
    mid = (alpha[0] * h1[...].astype(F32) + beta[0] * full[...]).astype(BF16).astype(F32)
    h2_out[...] = (mid * lax.rsqrt(jnp.mean(mid * mid, axis=-1, keepdims=True) + EPS) * g2[...]).astype(BF16)
    qs[...] = jnp.zeros_like(qs)

    def turn(z):
        return z * cosf[...] + pltpu.roll(z, 96, 1) * sina[...] + pltpu.roll(z, 32, 1) * sinb[...]

    for j in range(6):
        r = jnp.concatenate([wd[j, 0], wd[j, 1]], axis=1)
        z = jnp.dot(h2_out[...], r, preferred_element_type=F32)
        for kv in range(2):
            zk = z[:, kv * 128:(kv + 1) * 128]
            if j < 4:
                qs[kv, pl.ds(kv * 4 + j, 64, stride=8)] = turn(zk).astype(BF16).astype(F32)
            elif j == 4:
                kn[kv] = turn(zk).astype(BF16).astype(F32)
            else:
                vn[kv] = zk.astype(BF16).astype(F32)


def k2(o, gate, h1, onorm, w_out, g2, wattn, clen, alpha, beta):
    return pl.pallas_call(
        k2_body,
        out_shape=(jax.ShapeDtypeStruct(h1.shape, BF16), jax.ShapeDtypeStruct((2, 512, 128), F32),
                   jax.ShapeDtypeStruct((2, 64, 128), F32), jax.ShapeDtypeStruct((2, 64, 128), F32)),
        in_specs=[VMEM, VMEM, VMEM, VMEM, HBM, VMEM, HBM, SMEM, SMEM, SMEM],
        out_specs=(VMEM, VMEM, VMEM, VMEM),
        scratch_shapes=REDUCE_SCRATCH + [
            pltpu.VMEM((64, 1024), BF16), pltpu.VMEM((64, 128), F32), pltpu.VMEM((3, 64, 128), F32),
            pltpu.SemaphoreType.DMA((2, 3)),
            pltpu.VMEM((NAB, DA * 12, 128), BF16), pltpu.VMEM((DA * 12, 128), F32),
            pltpu.VMEM((6, 2, h1.shape[1], 128), BF16), pltpu.SemaphoreType.DMA((NAB,)),
            pltpu.VMEM((64, 128), F32), pltpu.VMEM((64, 128), F32), pltpu.VMEM((64, 128), F32)],
        compiler_params=pltpu.CompilerParams(vmem_limit_bytes=36 * 2 ** 20, collective_id=0, has_side_effects=True),
        cost_estimate=pl.CostEstimate(flops=int(6e10), bytes_accessed=int(2e7), transcendentals=0),
        name='mix_first')(o, gate, h1, onorm, w_out, g2, wattn, clen, alpha, beta)


NB3 = 8
NS3 = 4


def k3_body(kc, vc, qs, kn, vn, clen, k_out, v_out, attn, kb, vb, sscr, rsem, wsem):
    nstep = kc.shape[0] // NB3

    def reads(i, slot):
        return (pltpu.make_async_copy(vc.at[pl.ds(i * NB3, NB3)], vb.at[slot], rsem.at[slot, 1]),)

    def writes(i, slot):
        return (pltpu.make_async_copy(kb.at[slot], k_out.at[pl.ds(i * NB3, NB3)], wsem.at[slot, 0]),
                pltpu.make_async_copy(vb.at[slot], v_out.at[pl.ds(i * NB3, NB3)], wsem.at[slot, 1]))

    for i in range(NS3 - 1):
        for c in reads(i, i):
            c.start()

    def step(i, carry):
        slot = lax.rem(i, NS3)
        for c in reads(i, slot):
            c.wait()
        kb[slot] = kc[pl.ds(i * NB3, NB3)]
        row_id = lax.broadcasted_iota(jnp.int32, (16, 128), 0)
        for u in range(NB3):
            b = i * NB3 + u
            pos = clen[b]
            base = pl.multiple_of((pos // 16) * 16, 16)
            hit = row_id == pos - base
            for kv in range(2):
                for buf, new in ((kb, kn), (vb, vn)):
                    old = buf[slot, u, kv, pl.ds(base, 16)].astype(F32)
                    row = jnp.broadcast_to(new[kv, pl.ds(b, 1)], (16, 128))
                    buf[slot, u, kv, pl.ds(base, 16)] = jnp.where(hit, row, old).astype(BF16)
        for c in writes(i, slot):
            c.start()

        def score(h, carry):
            for u in range(NB3 // 2):
                w = h * (NB3 // 2) + u
                b = i * NB3 + w
                q = jnp.concatenate([qs[0, pl.ds(b * 8, 8)], qs[1, pl.ds(b * 8, 8)]], axis=1).astype(BF16)
                both = jnp.concatenate([kb[slot, w, 0], kb[slot, w, 1]], axis=1)
                s = lax.dot_general(q, both, (((1,), (1,)), ((), ())), preferred_element_type=F32)
                sscr[w] = s * (128 ** -0.5)
            return carry

        lax.fori_loop(0, 2, score, 0)
        tpos = lax.broadcasted_iota(jnp.int32, (8, 512), 1)
        for w in range(NB3):
            s = jnp.where(tpos <= clen[i * NB3 + w], sscr[w], -jnp.inf)
            e = jnp.exp(s - jnp.max(s, axis=-1, keepdims=True))
            sscr[w] = (e / jnp.sum(e, axis=-1, keepdims=True)).astype(BF16).astype(F32)
        lo = lax.broadcasted_iota(jnp.int32, (8, 128), 0) < 4

        def weigh(h, carry):
            for u in range(NB3 // 2):
                w = h * (NB3 // 2) + u
                b = i * NB3 + w
                both = jnp.concatenate([vb[slot, w, 0], vb[slot, w, 1]], axis=1)
                r = jnp.dot(sscr[w].astype(BF16), both, preferred_element_type=F32)
                attn[pl.ds(b * 8, 8)] = jnp.where(lo, r[:, :128], r[:, 128:]).astype(BF16).astype(F32)
            return carry

        lax.fori_loop(0, 2, weigh, 0)
        nxt = i + NS3 - 1

        @pl.when(nxt < nstep)
        def _():
            ps = lax.rem(nxt, NS3)

            @pl.when(i >= 1)
            def _():
                for c in writes(i - 1, ps):
                    c.wait()
            for c in reads(nxt, ps):
                c.start()
        return carry

    lax.fori_loop(0, nstep, step, 0)
    for i in range(nstep - NS3, nstep):
        for c in writes(i, i % NS3):
            c.wait()


def k3(kc, vc, qs, kn, vn, clen):
    shape = (NS3, NB3) + kc.shape[1:]
    return pl.pallas_call(
        k3_body,
        out_shape=(jax.ShapeDtypeStruct(kc.shape, BF16), jax.ShapeDtypeStruct(vc.shape, BF16),
                   jax.ShapeDtypeStruct((512, 128), F32)),
        in_specs=[VMEM, HBM, VMEM, VMEM, VMEM, SMEM],
        out_specs=(ANY, ANY, VMEM),
        scratch_shapes=[pltpu.VMEM(shape, BF16), pltpu.VMEM(shape, BF16), pltpu.VMEM((NB3, 8, 512), F32),
                        pltpu.SemaphoreType.DMA((NS3, 2)), pltpu.SemaphoreType.DMA((NS3, 2))],
        compiler_params=pltpu.CompilerParams(vmem_limit_bytes=20 * 2 ** 20),
        cost_estimate=pl.CostEstimate(flops=int(1e9), bytes_accessed=int(6e7), transcendentals=0),
        name='attention')(kc, vc, qs, kn, vn, clen)


def k4_body(attn, h2, w_out, alpha, beta, out,
            full, send_a, recv_a, own, recv_x, wo, sems, wosem, xin):
    wcopies = out_weight_copies(w_out, wo, wosem)
    for c in wcopies:
        c.start()
    for r in range(8):
        xin[:, r * 128:(r + 1) * 128] = attn[pl.ds(r, 64, stride=8)].astype(BF16)
    entry_barrier()
    reduce_over_tp(xin, wo, wcopies, full, send_a, recv_a, own, recv_x, sems, lambda j: None)
    out[...] = (alpha[1] * h2[...].astype(F32) + beta[1] * full[...]).astype(BF16)


def k4(attn, h2, w_out, alpha, beta):
    return pl.pallas_call(
        k4_body,
        out_shape=jax.ShapeDtypeStruct(h2.shape, BF16),
        in_specs=[VMEM, VMEM, HBM, SMEM, SMEM],
        out_specs=VMEM,
        scratch_shapes=REDUCE_SCRATCH + [pltpu.VMEM((64, 1024), BF16)],
        compiler_params=pltpu.CompilerParams(vmem_limit_bytes=20 * 2 ** 20, collective_id=1, has_side_effects=True),
        cost_estimate=pl.CostEstimate(flops=int(2e10), bytes_accessed=int(2e6), transcendentals=0),
        name='mix_second')(attn, h2, w_out, alpha, beta)


def solution(mesh):
    row_spec = P('dp', None)
    cache_spec = P('dp', 'tp', None, None)
    in_specs = (row_spec, P('dp'), cache_spec, cache_spec, cache_spec, P(None), P(None, None, 'tp', None),
                P(None, 'tp', None), P('tp'), P('tp', None), P('tp', None, None), P(None),
                P(None, 'tp', None, None), P('tp', None, None), P(None), P(None))
    out_specs = (row_spec, cache_spec, cache_spec, cache_spec)

    def local_step(hidden, cache_len, lin_state, k_cache, v_cache, norm_first, w_qkv, w_gate, slopes, out_norm,
                   w_out_lin, norm_second, w_attn, w_out_attn, mix_alpha, mix_beta):
        d = hidden.shape[1]

        def pin(x):
            return pltpu.with_memory_space_constraint(x, pltpu.HBM)
        state_out, o, gate, h1 = k1(pin(hidden), pin(norm_first.reshape(1, d)), pin(w_qkv.reshape(-1, 128)),
                                    pin(w_gate.reshape(-1, 128)), pin(slopes), pin(lin_state))
        wattn = pin(jnp.transpose(w_attn, (0, 2, 1, 3)).reshape(-1, 128))
        h2, qs, kn, vn = k2(o, gate, h1, out_norm, pin(w_out_lin.reshape(-1, d)), norm_second.reshape(1, d), wattn,
                            cache_len, mix_alpha, mix_beta)
        k_out, v_out, attn = k3(k_cache, pin(v_cache), qs, kn, vn, cache_len)
        hidden_out = k4(attn, h2, pin(w_out_attn.reshape(-1, d)), mix_alpha, mix_beta)
        return hidden_out, state_out, k_out, v_out

    return jax.shard_map(local_step, mesh=mesh, in_specs=in_specs, out_specs=out_specs, check_vma=False)
```

```python
import math
import jax
import jax.numpy as jnp
from jax import lax
from jax.experimental import pallas as pl
from jax.experimental.pallas import tpu as pltpu
from jax.sharding import PartitionSpec as P

EPS = 1e-5
ROPE_BASE = 10000000.0
F32 = jnp.float32
BF16 = jnp.bfloat16
MESH = pl.DeviceIdType.MESH
ANY = pl.BlockSpec(memory_space=pl.ANY)
HBM = pl.BlockSpec(memory_space=pltpu.HBM)
VMEM = pl.BlockSpec(memory_space=pltpu.VMEM)
SMEM = pl.BlockSpec(memory_space=pltpu.SMEM)

DC = 256
RS = 9 * DC + 16
NWB = 5
NSB = 23
LAG = 2
LATE = 17


def k1_body(hid_hbm, g1_hbm, wqkv, wgate, slopes_hbm, lin, st_out, o_out, gate_out, h1_out,
            wbuf, gbuf, scr, acc, qq, kk, vv, sbuf, hid, g1, slopes, wsem, rsem, ssem, msem):
    nchunk = hid.shape[1] // DC
    small = [pltpu.make_async_copy(src, dst, msem.at[n])
             for n, (src, dst) in enumerate(((hid_hbm, hid), (g1_hbm, g1), (slopes_hbm, slopes)))]
    for c in small:
        c.start()

    def wcopies(i, slot):
        return (pltpu.make_async_copy(wqkv.at[pl.ds(i * (DC * 24), DC * 24)], wbuf.at[slot], wsem.at[slot, 0]),
                pltpu.make_async_copy(wgate.at[pl.ds(i * (DC * 8), DC * 8)], gbuf.at[slot], wsem.at[slot, 1]))

    def sread(j, slot):
        hp, bb = j // 8, lax.rem(j, 8)
        return pltpu.make_async_copy(lin.at[pl.ds(bb * 8, 8), pl.ds(hp * 2, 2)], sbuf.at[slot], rsem.at[slot])

    def swrite(j, slot):
        hp, bb = j // 8, lax.rem(j, 8)
        return pltpu.make_async_copy(sbuf.at[slot], st_out.at[pl.ds(bb * 8, 8), pl.ds(hp * 2, 2)], ssem.at[slot])

    for i in range(NWB):
        for c in wcopies(i, i):
            c.start()
    for c in small:
        c.wait()
    x = hid[...].astype(F32)
    h1_out[...] = (x * lax.rsqrt(jnp.mean(x * x, axis=-1, keepdims=True) + EPS) * g1[...]).astype(BF16)
    acc[...] = jnp.zeros_like(acc)

    def wstep(i, carry):
        slot = lax.rem(i, NWB)
        for c in wcopies(i, slot):
            c.wait()
        for d2 in range(0, DC, 2):
            t = wbuf[slot, pl.ds(d2 * 24, 48)].astype(F32)
            for u in range(6):
                scr[pl.ds((u % 3) * RS + 9 * (d2 + u // 3), 8, stride=2)] = t[u * 8:(u + 1) * 8]
            t = gbuf[slot, pl.ds(d2 * 8, 16)].astype(F32)
            for u in range(2):
                scr[pl.ds(3 * RS + 9 * (d2 + u), 8, stride=2)] = t[u * 8:(u + 1) * 8]
        hh = h1_out[:, pl.ds(pl.multiple_of(i * DC, DC), DC)]

        def head(m):
            return scr[pl.ds((m // 8) * RS + 2 * (m % 8), DC, stride=9)]

        for n in range(16):
            r = jnp.concatenate([head(2 * n), head(2 * n + 1)], axis=1).astype(BF16)
            acc[:, n * 256:(n + 1) * 256] += jnp.dot(hh, r, preferred_element_type=F32)

        @pl.when(i + NWB < nchunk)
        def _():
            for c in wcopies(i + NWB, slot):
                c.start()

        sread(i, i).start()

        @pl.when(i >= LATE)
        def _():
            sread(i - LATE + nchunk, i - LATE + nchunk).start()
        return carry

    lax.fori_loop(0, nchunk, wstep, 0)

    for hp in range(4):
        def pair(c):
            base = c * 1024 + hp * 256
            return jnp.concatenate([acc[:, base:base + 128], acc[:, base + 128:base + 256]], axis=0)

        def act(c):
            z = pair(c)
            return (z * jax.nn.sigmoid(z)).astype(BF16).astype(F32)
        qq[hp] = act(0)
        kk[hp] = act(1)
        vv[hp] = act(2)
        g = jax.nn.sigmoid(pair(3))
        gate_out[2 * hp] = g[:64]
        gate_out[2 * hp + 1] = g[64:]

    def sstep(j, carry):
        hp, bb = j // 8, lax.rem(j, 8)
        slot = lax.rem(j, NSB)
        sread(j, slot).wait()
        rid = lax.broadcasted_iota(jnp.int32, (16, 128), 0)
        for p in range(2):
            decay = jnp.exp(jnp.full((8, 128), -slopes[hp * 2 + p], F32))[0:1]
            at = pl.ds(p * 64 + bb * 8, 8)
            kq = jnp.concatenate([kk[hp, at], qq[hp, at]], axis=0).T.astype(BF16)
            v16 = jnp.concatenate([vv[hp, at], jnp.zeros((8, 128), F32)], axis=0)
            rows = []
            for i in range(8):
                pick = jnp.concatenate([jnp.where(rid == i, v16, 0.0), jnp.where(rid == 8 + i, 1.0, 0.0)], axis=1)
                both = jnp.dot(kq, pick.astype(BF16), preferred_element_type=F32)
                s_new = decay * sbuf[slot, i, p] + both[:, :128]
                sbuf[slot, i, p] = s_new
                rows.append(jnp.sum(both[:, 128:] * s_new, axis=0, keepdims=True))
            o_out[hp * 2 + p, pl.ds(bb * 8, 8)] = jnp.concatenate(rows, axis=0)
        swrite(j, slot).start()

        @pl.when((j >= LAG) & (j - LAG + NSB < 32))
        def _():
            jj = j - LAG
            ps = lax.rem(jj, NSB)
            swrite(jj, ps).wait()
            sread(jj + NSB, ps).start()
        return carry

    lax.fori_loop(0, 32, sstep, 0)
    for j in range(32 - NSB, 32):
        swrite(j, j % NSB).wait()


def k1(hidden, g1, wqkv, wgate, slopes, lin):
    return pl.pallas_call(
        k1_body,
        out_shape=(jax.ShapeDtypeStruct(lin.shape, F32), jax.ShapeDtypeStruct((8, 64, 128), F32),
                   jax.ShapeDtypeStruct((8, 64, 128), F32), jax.ShapeDtypeStruct(hidden.shape, BF16)),
        in_specs=[HBM] * 6,
        out_specs=(ANY, VMEM, VMEM, VMEM),
        scratch_shapes=[
            pltpu.VMEM((NWB, DC * 24, 128), BF16), pltpu.VMEM((NWB, DC * 8, 128), BF16),
            pltpu.VMEM((4 * RS, 128), F32), pltpu.VMEM((64, 4096), F32),
            pltpu.VMEM((4, 128, 128), F32), pltpu.VMEM((4, 128, 128), F32), pltpu.VMEM((4, 128, 128), F32),
            pltpu.VMEM((NSB, 8, 2, 128, 128), F32),
            pltpu.VMEM(hidden.shape, BF16), pltpu.VMEM(g1.shape, F32), pltpu.SMEM(slopes.shape, F32),
            pltpu.SemaphoreType.DMA((NWB, 2)), pltpu.SemaphoreType.DMA((NSB,)), pltpu.SemaphoreType.DMA((NSB,)),
            pltpu.SemaphoreType.DMA((3,))],
        compiler_params=pltpu.CompilerParams(vmem_limit_bytes=45 * 2 ** 20),
        cost_estimate=pl.CostEstimate(flops=int(1e12), bytes_accessed=int(1.1e8), transcendentals=0),
        name='lightning')(hidden, g1, wqkv, wgate, slopes, lin)


NB3 = 8
NS3 = 4
NPRE = 3

NCH = 5
CW = 512
HALF = NCH * CW


def entry_barrier():
    tp = lax.axis_index('tp')
    bar = pltpu.get_barrier_semaphore()
    for peer in peers(tp):
        pl.semaphore_signal(bar, inc=1, device_id={'tp': peer}, device_id_type=MESH)
    pl.semaphore_wait(bar, 3)


def peers(tp):
    core = lax.rem(tp, 2)
    partner = tp + 1 - 2 * core
    across = lax.rem(tp + 2, 4)
    diag = lax.rem(partner + 2, 4)
    return partner, across, diag


def out_weight_copies(w, wo, wosem):
    core = lax.rem(lax.axis_index('tp'), 2)
    out = []
    for s in range(2 * NCH):
        side = core if s % 2 else 1 - core
        col = pl.multiple_of(side * HALF + (s // 2) * CW, CW)
        slot = s % wo.shape[0]
        out.append(pltpu.make_async_copy(w.at[:, pl.ds(col, CW)], wo.at[slot], wosem.at[slot]))
    return out


def reduce_over_tp(xin, wo, wcopies, full, send_a, recv_a, own, recv_x, sems, between):
    tp = lax.axis_index('tp')
    core = lax.rem(tp, 2)
    partner, across, _ = peers(tp)

    def rcopy(src, dst, k, j, dev):
        return pltpu.make_async_remote_copy(src_ref=src, dst_ref=dst, send_sem=sems.at[k, j],
                                            recv_sem=sems.at[k + 1, j], device_id={'tp': dev}, device_id_type=MESH)
    ca = [rcopy(send_a.at[j], recv_a.at[j], 0, j, partner) for j in range(NCH)]
    cx = [rcopy(own.at[j], recv_x.at[j], 2, j, across) for j in range(NCH)]
    cf = []
    for j in range(NCH):
        col = pl.multiple_of(core * HALF + j * CW, CW)
        cf.append(rcopy(full.at[:, pl.ds(col, CW)], full.at[:, pl.ds(col, CW)], 4, j, partner))

    def product(n):
        wcopies[n].wait()
        out = jnp.dot(xin[...], wo[n % wo.shape[0]], preferred_element_type=F32)
        if n + wo.shape[0] < 2 * NCH:
            wcopies[n + wo.shape[0]].start()
        return out

    def combine(j):
        ca[j].wait_recv()
        own[j] = own[j] + recv_a[j]
        cx[j].start()

    for j in range(NCH):
        send_a[j] = product(2 * j)
        ca[j].start()
        own[j] = product(2 * j + 1)
        if j:
            combine(j - 1)
    combine(NCH - 1)
    for j in range(NCH):
        between(j)
        cx[j].wait_recv()
        col = pl.multiple_of(core * HALF + j * CW, CW)
        full[:, pl.ds(col, CW)] = own[j] + recv_x[j]
        cf[j].start()
    for j in range(NCH):
        cf[j].wait_recv()
    for j in range(NCH):
        ca[j].wait_send()
        cx[j].wait_send()
        cf[j].wait_send()


def reduce_scratch(slots):
    chunk = pltpu.VMEM((NCH, 64, CW), F32)
    return [pltpu.VMEM((64, 2 * HALF), F32), chunk, chunk, chunk, chunk, pltpu.VMEM((slots, 1024, CW), BF16),
            pltpu.SemaphoreType.DMA((6, NCH)), pltpu.SemaphoreType.DMA((slots,))]


NAB = 8
DA = 128


def k2_body(o_in, gate_in, h1, onorm, w_out, g2, wattn, clen, alpha, beta, vc,
            h2_out, qs, kn, vn, vpre,
            full, send_a, recv_a, own, recv_x, wo, sems, wosem,
            xin, ssl, ssr, sssem, abuf, ascr, wd, asem, cosf, sina, sinb, vsem):
    tp = lax.axis_index('tp')
    nchunk = h1.shape[1] // DA
    wcopies = out_weight_copies(w_out, wo, wosem)
    for c in wcopies[:wo.shape[0]]:
        c.start()

    def acopy(i, slot):
        return pltpu.make_async_copy(wattn.at[pl.ds(i * (DA * 12), DA * 12)], abuf.at[slot], asem.at[slot])
    for i in range(NAB):
        acopy(i, i).start()
    sq = jnp.zeros((64, 128), F32)
    for h in range(8):
        sq = sq + o_in[h] * o_in[h]
    wide = jnp.concatenate([sq, jnp.zeros((64, 128), F32)], axis=0).T
    ssl[...] = jnp.broadcast_to(jnp.sum(wide, axis=0, keepdims=True), (8, 128))
    entry_barrier()
    copies = [pltpu.make_async_remote_copy(src_ref=ssl, dst_ref=ssr.at[k], send_sem=sssem.at[0, k],
                                           recv_sem=sssem.at[1, k], device_id={'tp': dev}, device_id_type=MESH)
              for k, dev in enumerate(peers(tp))]
    for c in copies:
        c.start()
    def spread(b, carry):
        cosf[pl.ds(b, 1)] = jnp.full((1, 128), clen[b].astype(F32), F32)
        return carry

    lax.fori_loop(0, 64, spread, 0)
    lane = lax.broadcasted_iota(jnp.int32, (64, 128), 1)
    power = (lane & 31).astype(F32) * (-2.0 / 64)
    angle = cosf[...] * jnp.exp(power * math.log(ROPE_BASE))
    sine = jnp.sin(angle)
    cosf[...] = jnp.where(lane < 64, jnp.cos(angle), 1.0)
    sina[...] = jnp.where(lane < 32, -sine, 0.0)
    sinb[...] = jnp.where((lane >= 32) & (lane < 64), sine, 0.0)
    for c in copies:
        c.wait_recv()
    total = jnp.broadcast_to(((ssl[...] + ssr[0]) + (ssr[1] + ssr[2]))[0:1], (128, 128)).T[:64]
    inv = lax.rsqrt(total / 4096.0 + EPS)
    for h in range(8):
        xin[:, h * 128:(h + 1) * 128] = (o_in[h] * inv * onorm[h:h + 1] * gate_in[h]).astype(BF16)

    def demix(i, carry):
        slot = lax.rem(i, NAB)
        acopy(i, slot).wait()
        ascr[...] = abuf[slot].astype(F32)
        for j in range(6):
            for kv in range(2):
                wd[j, kv, pl.ds(pl.multiple_of(i * DA, DA), DA)] = ascr[pl.ds(2 * j + kv, DA, stride=12)].astype(BF16)

        @pl.when(i + NAB < nchunk)
        def _():
            acopy(i + NAB, slot).start()
        return carry

    vcopy = pltpu.make_async_copy(vc.at[pl.ds(0, NPRE * NB3)], vpre, vsem)

    def between(j):
        if j == 0:
            vcopy.start()
        lax.fori_loop(j * (nchunk // NCH), (j + 1) * (nchunk // NCH), demix, 0)

    reduce_over_tp(xin, wo, wcopies, full, send_a, recv_a, own, recv_x, sems, between)
    for c in copies:
        c.wait_send()
    vcopy.wait()
    mid = (alpha[0] * h1[...].astype(F32) + beta[0] * full[...]).astype(BF16).astype(F32)
    h2_out[...] = (mid * lax.rsqrt(jnp.mean(mid * mid, axis=-1, keepdims=True) + EPS) * g2[...]).astype(BF16)
    qs[...] = jnp.zeros_like(qs)

    def turn(z):
        return z * cosf[...] + pltpu.roll(z, 96, 1) * sina[...] + pltpu.roll(z, 32, 1) * sinb[...]

    for j in range(6):
        r = jnp.concatenate([wd[j, 0], wd[j, 1]], axis=1)
        z = jnp.dot(h2_out[...], r, preferred_element_type=F32)
        for kv in range(2):
            zk = z[:, kv * 128:(kv + 1) * 128]
            if j < 4:
                qs[kv, pl.ds(kv * 4 + j, 64, stride=8)] = turn(zk).astype(BF16).astype(F32)
            elif j == 4:
                kn[kv] = turn(zk).astype(BF16).astype(F32)
            else:
                vn[kv] = zk.astype(BF16).astype(F32)


def k2(o, gate, h1, onorm, w_out, g2, wattn, clen, alpha, beta, vc):
    return pl.pallas_call(
        k2_body,
        out_shape=(jax.ShapeDtypeStruct(h1.shape, BF16), jax.ShapeDtypeStruct((2, 512, 128), F32),
                   jax.ShapeDtypeStruct((2, 64, 128), F32), jax.ShapeDtypeStruct((2, 64, 128), F32),
                   jax.ShapeDtypeStruct((NPRE * NB3,) + vc.shape[1:], BF16)),
        in_specs=[VMEM, VMEM, VMEM, VMEM, HBM, VMEM, HBM, SMEM, SMEM, SMEM, HBM],
        out_specs=(VMEM,) * 5,
        scratch_shapes=reduce_scratch(4) + [
            pltpu.VMEM((64, 1024), BF16), pltpu.VMEM((8, 128), F32), pltpu.VMEM((3, 8, 128), F32),
            pltpu.SemaphoreType.DMA((2, 3)),
            pltpu.VMEM((NAB, DA * 12, 128), BF16), pltpu.VMEM((DA * 12, 128), F32),
            pltpu.VMEM((6, 2, h1.shape[1], 128), BF16), pltpu.SemaphoreType.DMA((NAB,)),
            pltpu.VMEM((64, 128), F32), pltpu.VMEM((64, 128), F32), pltpu.VMEM((64, 128), F32),
            pltpu.SemaphoreType.DMA],
        compiler_params=pltpu.CompilerParams(vmem_limit_bytes=29 * 2 ** 20, collective_id=0, has_side_effects=True),
        cost_estimate=pl.CostEstimate(flops=int(6e10), bytes_accessed=int(2e7), transcendentals=0),
        name='mix_first')(o, gate, h1, onorm, w_out, g2, wattn, clen, alpha, beta, vc)


def k3_body(kc, vc, vpre, qs, kn, vn, clen, k_out, v_out, attn, kb, vb, sscr, rsem, wsem):
    nstep = kc.shape[0] // NB3

    def reads(i, slot):
        return (pltpu.make_async_copy(vc.at[pl.ds(i * NB3, NB3)], vb.at[slot], rsem.at[slot, 1]),)

    def writes(i, slot):
        return (pltpu.make_async_copy(kb.at[slot], k_out.at[pl.ds(i * NB3, NB3)], wsem.at[slot, 0]),
                pltpu.make_async_copy(vb.at[slot], v_out.at[pl.ds(i * NB3, NB3)], wsem.at[slot, 1]))

    for i in range(NPRE, NS3):
        for c in reads(i, i):
            c.start()

    def step(i, carry):
        slot = lax.rem(i, NS3)

        @pl.when(i < NPRE)
        def _():
            vb[slot] = vpre[pl.ds(pl.multiple_of(jnp.minimum(i, NPRE - 1) * NB3, NB3), NB3)]

        @pl.when(i >= NPRE)
        def _():
            for c in reads(i, slot):
                c.wait()
        kb[slot] = kc[pl.ds(i * NB3, NB3)]
        row_id = lax.broadcasted_iota(jnp.int32, (16, 128), 0)
        for u in range(NB3):
            b = i * NB3 + u
            pos = clen[b]
            base = pl.multiple_of((pos // 16) * 16, 16)
            hit = row_id == pos - base
            for kv in range(2):
                for buf, new in ((kb, kn), (vb, vn)):
                    old = buf[slot, u, kv, pl.ds(base, 16)].astype(F32)
                    row = jnp.broadcast_to(new[kv, pl.ds(b, 1)], (16, 128))
                    buf[slot, u, kv, pl.ds(base, 16)] = jnp.where(hit, row, old).astype(BF16)
        for c in writes(i, slot):
            c.start()

        def score(h, carry):
            for u in range(NB3 // 2):
                w = h * (NB3 // 2) + u
                b = i * NB3 + w
                q = jnp.concatenate([qs[0, pl.ds(b * 8, 8)], qs[1, pl.ds(b * 8, 8)]], axis=1).astype(BF16)
                both = jnp.concatenate([kb[slot, w, 0], kb[slot, w, 1]], axis=1)
                s = lax.dot_general(q, both, (((1,), (1,)), ((), ())), preferred_element_type=F32)
                sscr[w] = s * (128 ** -0.5)
            return carry

        lax.fori_loop(0, 2, score, 0)
        tpos = lax.broadcasted_iota(jnp.int32, (8, 512), 1)
        for w in range(NB3):
            s = jnp.where(tpos <= clen[i * NB3 + w], sscr[w], -jnp.inf)
            e = jnp.exp(s - jnp.max(s, axis=-1, keepdims=True))
            sscr[w] = (e / jnp.sum(e, axis=-1, keepdims=True)).astype(BF16).astype(F32)
        lo = lax.broadcasted_iota(jnp.int32, (8, 128), 0) < 4

        def weigh(h, carry):
            for u in range(NB3 // 2):
                w = h * (NB3 // 2) + u
                b = i * NB3 + w
                both = jnp.concatenate([vb[slot, w, 0], vb[slot, w, 1]], axis=1)
                r = jnp.dot(sscr[w].astype(BF16), both, preferred_element_type=F32)
                attn[pl.ds(b * 8, 8)] = jnp.where(lo, r[:, :128], r[:, 128:]).astype(BF16).astype(F32)
            return carry

        lax.fori_loop(0, 2, weigh, 0)
        nxt = i + NS3 - 1

        @pl.when((i >= 1) & (nxt < nstep))
        def _():
            ps = lax.rem(nxt, NS3)
            for c in writes(i - 1, ps):
                c.wait()
            for c in reads(nxt, ps):
                c.start()
        return carry

    lax.fori_loop(0, nstep, step, 0)
    for i in range(nstep - NS3, nstep):
        for c in writes(i, i % NS3):
            c.wait()


def k3(kc, vc, vpre, qs, kn, vn, clen):
    shape = (NS3, NB3) + kc.shape[1:]
    return pl.pallas_call(
        k3_body,
        out_shape=(jax.ShapeDtypeStruct(kc.shape, BF16), jax.ShapeDtypeStruct(vc.shape, BF16),
                   jax.ShapeDtypeStruct((512, 128), F32)),
        in_specs=[VMEM, HBM, VMEM, VMEM, VMEM, VMEM, SMEM],
        out_specs=(ANY, ANY, VMEM),
        scratch_shapes=[pltpu.VMEM(shape, BF16), pltpu.VMEM(shape, BF16), pltpu.VMEM((NB3, 8, 512), F32),
                        pltpu.SemaphoreType.DMA((NS3, 2)), pltpu.SemaphoreType.DMA((NS3, 2))],
        compiler_params=pltpu.CompilerParams(vmem_limit_bytes=24 * 2 ** 20),
        cost_estimate=pl.CostEstimate(flops=int(1e9), bytes_accessed=int(6e7), transcendentals=0),
        name='attention')(kc, vc, vpre, qs, kn, vn, clen)


def k4_body(attn, h2, w_out, alpha, beta, out,
            full, send_a, recv_a, own, recv_x, wo, sems, wosem, xin):
    wcopies = out_weight_copies(w_out, wo, wosem)
    for c in wcopies[:wo.shape[0]]:
        c.start()
    for r in range(8):
        xin[:, r * 128:(r + 1) * 128] = attn[pl.ds(r, 64, stride=8)].astype(BF16)
    entry_barrier()
    reduce_over_tp(xin, wo, wcopies, full, send_a, recv_a, own, recv_x, sems, lambda j: None)
    out[...] = (alpha[1] * h2[...].astype(F32) + beta[1] * full[...]).astype(BF16)


def k4(attn, h2, w_out, alpha, beta):
    return pl.pallas_call(
        k4_body,
        out_shape=jax.ShapeDtypeStruct(h2.shape, BF16),
        in_specs=[VMEM, VMEM, HBM, SMEM, SMEM],
        out_specs=VMEM,
        scratch_shapes=reduce_scratch(2 * NCH) + [pltpu.VMEM((64, 1024), BF16)],
        compiler_params=pltpu.CompilerParams(vmem_limit_bytes=20 * 2 ** 20, collective_id=1, has_side_effects=True),
        cost_estimate=pl.CostEstimate(flops=int(2e10), bytes_accessed=int(2e6), transcendentals=0),
        name='mix_second')(attn, h2, w_out, alpha, beta)


def solution(mesh):
    row_spec = P('dp', None)
    cache_spec = P('dp', 'tp', None, None)
    in_specs = (row_spec, P('dp'), cache_spec, cache_spec, cache_spec, P(None), P(None, None, 'tp', None),
                P(None, 'tp', None), P('tp'), P('tp', None), P('tp', None, None), P(None),
                P(None, 'tp', None, None), P('tp', None, None), P(None), P(None))
    out_specs = (row_spec, cache_spec, cache_spec, cache_spec)

    def local_step(hidden, cache_len, lin_state, k_cache, v_cache, norm_first, w_qkv, w_gate, slopes, out_norm,
                   w_out_lin, norm_second, w_attn, w_out_attn, mix_alpha, mix_beta):
        d = hidden.shape[1]

        def pin(x):
            return pltpu.with_memory_space_constraint(x, pltpu.HBM)
        state_out, o, gate, h1 = k1(pin(hidden), pin(norm_first.reshape(1, d)), pin(w_qkv.reshape(-1, 128)),
                                    pin(w_gate.reshape(-1, 128)), pin(slopes), pin(lin_state))
        pinned_v = pin(v_cache)
        wattn = pin(jnp.transpose(w_attn, (0, 2, 1, 3)).reshape(-1, 128))
        h2, qs, kn, vn, vpre = k2(o, gate, h1, out_norm, pin(w_out_lin.reshape(-1, d)), norm_second.reshape(1, d), wattn,
                            cache_len, mix_alpha, mix_beta, pinned_v)
        k_out, v_out, attn = k3(k_cache, pinned_v, vpre, qs, kn, vn, cache_len)
        hidden_out = k4(attn, h2, pin(w_out_attn.reshape(-1, d)), mix_alpha, mix_beta)
        return hidden_out, state_out, k_out, v_out

    return jax.shard_map(local_step, mesh=mesh, in_specs=in_specs, out_specs=out_specs, check_vma=False)
```

```python
import math
import jax
import jax.numpy as jnp
from jax import lax
from jax.experimental import pallas as pl
from jax.experimental.pallas import tpu as pltpu
from jax.sharding import PartitionSpec as P

EPS = 1e-5
ROPE_BASE = 10000000.0
F32 = jnp.float32
BF16 = jnp.bfloat16
MESH = pl.DeviceIdType.MESH
ANY = pl.BlockSpec(memory_space=pl.ANY)
HBM = pl.BlockSpec(memory_space=pltpu.HBM)
VMEM = pl.BlockSpec(memory_space=pltpu.VMEM)
SMEM = pl.BlockSpec(memory_space=pltpu.SMEM)

DC = 256
RS = 9 * DC + 16
NWB = 5
NSB = 23
LAG = 2
LATE = 17


def k1_body(hid_hbm, g1_hbm, wqkv, wgate, slopes_hbm, lin, st_out, o_out, gate_out, h1_out,
            wbuf, gbuf, scr, acc, qq, kk, vv, sbuf, hid, g1, slopes, wsem, rsem, ssem, msem):
    nchunk = hid.shape[1] // DC
    small = [pltpu.make_async_copy(src, dst, msem.at[n])
             for n, (src, dst) in enumerate(((hid_hbm, hid), (g1_hbm, g1), (slopes_hbm, slopes)))]
    for c in small:
        c.start()

    def wcopies(i, slot):
        return (pltpu.make_async_copy(wqkv.at[pl.ds(i * (DC * 24), DC * 24)], wbuf.at[slot], wsem.at[slot, 0]),
                pltpu.make_async_copy(wgate.at[pl.ds(i * (DC * 8), DC * 8)], gbuf.at[slot], wsem.at[slot, 1]))

    def sread(j, slot):
        hp, bb = j // 8, lax.rem(j, 8)
        return pltpu.make_async_copy(lin.at[pl.ds(bb * 8, 8), pl.ds(hp * 2, 2)], sbuf.at[slot], rsem.at[slot])

    def swrite(j, slot):
        hp, bb = j // 8, lax.rem(j, 8)
        return pltpu.make_async_copy(sbuf.at[slot], st_out.at[pl.ds(bb * 8, 8), pl.ds(hp * 2, 2)], ssem.at[slot])

    for i in range(NWB):
        for c in wcopies(i, i):
            c.start()
    for c in small:
        c.wait()
    x = hid[...].astype(F32)
    h1_out[...] = (x * lax.rsqrt(jnp.mean(x * x, axis=-1, keepdims=True) + EPS) * g1[...]).astype(BF16)
    acc[...] = jnp.zeros_like(acc)

    def wstep(i, carry):
        slot = lax.rem(i, NWB)
        for c in wcopies(i, slot):
            c.wait()
        for d2 in range(0, DC, 2):
            t = wbuf[slot, pl.ds(d2 * 24, 48)].astype(F32)
            for u in range(6):
                scr[pl.ds((u % 3) * RS + 9 * (d2 + u // 3), 8, stride=2)] = t[u * 8:(u + 1) * 8]
            t = gbuf[slot, pl.ds(d2 * 8, 16)].astype(F32)
            for u in range(2):
                scr[pl.ds(3 * RS + 9 * (d2 + u), 8, stride=2)] = t[u * 8:(u + 1) * 8]
        hh = h1_out[:, pl.ds(pl.multiple_of(i * DC, DC), DC)]

        def head(m):
            return scr[pl.ds((m // 8) * RS + 2 * (m % 8), DC, stride=9)]

        for n in range(16):
            r = jnp.concatenate([head(2 * n), head(2 * n + 1)], axis=1).astype(BF16)
            acc[:, n * 256:(n + 1) * 256] += jnp.dot(hh, r, preferred_element_type=F32)

        @pl.when(i + NWB < nchunk)
        def _():
            for c in wcopies(i + NWB, slot):
                c.start()

        sread(i, i).start()

        @pl.when(i >= LATE)
        def _():
            sread(i - LATE + nchunk, i - LATE + nchunk).start()
        return carry

    lax.fori_loop(0, nchunk, wstep, 0)

    for hp in range(4):
        def pair(c):
            base = c * 1024 + hp * 256
            return jnp.concatenate([acc[:, base:base + 128], acc[:, base + 128:base + 256]], axis=0)

        def act(c):
            z = pair(c)
            return (z * jax.nn.sigmoid(z)).astype(BF16).astype(F32)
        qq[hp] = act(0)
        kk[hp] = act(1)
        vv[hp] = act(2)
        g = jax.nn.sigmoid(pair(3))
        gate_out[2 * hp] = g[:64]
        gate_out[2 * hp + 1] = g[64:]

    def sstep(j, carry):
        hp, bb = j // 8, lax.rem(j, 8)
        slot = lax.rem(j, NSB)
        sread(j, slot).wait()
        rid = lax.broadcasted_iota(jnp.int32, (16, 128), 0)
        for p in range(2):
            decay = jnp.exp(jnp.full((8, 128), -slopes[hp * 2 + p], F32))[0:1]
            at = pl.ds(p * 64 + bb * 8, 8)
            kq = jnp.concatenate([kk[hp, at], qq[hp, at]], axis=0).T.astype(BF16)
            v16 = jnp.concatenate([vv[hp, at], jnp.zeros((8, 128), F32)], axis=0)
            rows = []
            for i in range(8):
                pick = jnp.concatenate([jnp.where(rid == i, v16, 0.0), jnp.where(rid == 8 + i, 1.0, 0.0)], axis=1)
                both = jnp.dot(kq, pick.astype(BF16), preferred_element_type=F32)
                s_new = decay * sbuf[slot, i, p] + both[:, :128]
                sbuf[slot, i, p] = s_new
                rows.append(jnp.sum(both[:, 128:] * s_new, axis=0, keepdims=True))
            o_out[hp * 2 + p, pl.ds(bb * 8, 8)] = jnp.concatenate(rows, axis=0)
        swrite(j, slot).start()

        @pl.when((j >= LAG) & (j - LAG + NSB < 32))
        def _():
            jj = j - LAG
            ps = lax.rem(jj, NSB)
            swrite(jj, ps).wait()
            sread(jj + NSB, ps).start()
        return carry

    lax.fori_loop(0, 32, sstep, 0)
    for j in range(32 - NSB, 32):
        swrite(j, j % NSB).wait()


def k1(hidden, g1, wqkv, wgate, slopes, lin):
    return pl.pallas_call(
        k1_body,
        out_shape=(jax.ShapeDtypeStruct(lin.shape, F32), jax.ShapeDtypeStruct((8, 64, 128), F32),
                   jax.ShapeDtypeStruct((8, 64, 128), F32), jax.ShapeDtypeStruct(hidden.shape, BF16)),
        in_specs=[HBM] * 6,
        out_specs=(ANY, VMEM, VMEM, VMEM),
        scratch_shapes=[
            pltpu.VMEM((NWB, DC * 24, 128), BF16), pltpu.VMEM((NWB, DC * 8, 128), BF16),
            pltpu.VMEM((4 * RS, 128), F32), pltpu.VMEM((64, 4096), F32),
            pltpu.VMEM((4, 128, 128), F32), pltpu.VMEM((4, 128, 128), F32), pltpu.VMEM((4, 128, 128), F32),
            pltpu.VMEM((NSB, 8, 2, 128, 128), F32),
            pltpu.VMEM(hidden.shape, BF16), pltpu.VMEM(g1.shape, F32), pltpu.SMEM(slopes.shape, F32),
            pltpu.SemaphoreType.DMA((NWB, 2)), pltpu.SemaphoreType.DMA((NSB,)), pltpu.SemaphoreType.DMA((NSB,)),
            pltpu.SemaphoreType.DMA((3,))],
        compiler_params=pltpu.CompilerParams(vmem_limit_bytes=45 * 2 ** 20),
        cost_estimate=pl.CostEstimate(flops=int(1e12), bytes_accessed=int(1.1e8), transcendentals=0),
        name='lightning')(hidden, g1, wqkv, wgate, slopes, lin)


NB3 = 8
NS3 = 4
NPRE = 3

NCH = 5
CW = 512
HALF = NCH * CW


def entry_barrier():
    tp = lax.axis_index('tp')
    bar = pltpu.get_barrier_semaphore()
    for peer in peers(tp):
        pl.semaphore_signal(bar, inc=1, device_id={'tp': peer}, device_id_type=MESH)
    pl.semaphore_wait(bar, 3)


def peers(tp):
    core = lax.rem(tp, 2)
    partner = tp + 1 - 2 * core
    across = lax.rem(tp + 2, 4)
    diag = lax.rem(partner + 2, 4)
    return partner, across, diag


def out_weight_copies(w, wo, wosem):
    core = lax.rem(lax.axis_index('tp'), 2)
    out = []
    for s in range(2 * NCH):
        side = core if s % 2 else 1 - core
        col = pl.multiple_of(side * HALF + (s // 2) * CW, CW)
        slot = s % wo.shape[0]
        out.append(pltpu.make_async_copy(w.at[:, pl.ds(col, CW)], wo.at[slot], wosem.at[slot]))
    return out


def reduce_over_tp(xin, wo, wcopies, full, send_a, recv_a, own, recv_x, sems, between, emit):
    tp = lax.axis_index('tp')
    core = lax.rem(tp, 2)
    partner, across, _ = peers(tp)

    def rcopy(src, dst, k, j, dev):
        return pltpu.make_async_remote_copy(src_ref=src, dst_ref=dst, send_sem=sems.at[k, j],
                                            recv_sem=sems.at[k + 1, j], device_id={'tp': dev}, device_id_type=MESH)
    ca = [rcopy(send_a.at[j], recv_a.at[j], 0, j, partner) for j in range(NCH)]
    cx = [rcopy(own.at[j], recv_x.at[j], 2, j, across) for j in range(NCH)]
    cf = []
    for j in range(NCH):
        col = pl.multiple_of(core * HALF + j * CW, CW)
        cf.append(rcopy(full.at[:, pl.ds(col, CW)], full.at[:, pl.ds(col, CW)], 4, j, partner))

    def product(n):
        wcopies[n].wait()
        out = jnp.dot(xin[...], wo[n % wo.shape[0]], preferred_element_type=F32)
        if n + wo.shape[0] < 2 * NCH:
            wcopies[n + wo.shape[0]].start()
        return out

    def combine(j):
        ca[j].wait_recv()
        own[j] = own[j] + recv_a[j]
        cx[j].start()

    for j in range(NCH):
        send_a[j] = product(2 * j)
        ca[j].start()
        own[j] = product(2 * j + 1)
        if j:
            combine(j - 1)
    combine(NCH - 1)
    for j in range(NCH):
        between(j)
        cx[j].wait_recv()
        col = pl.multiple_of(core * HALF + j * CW, CW)
        full[:, pl.ds(col, CW)] = own[j] + recv_x[j]
        cf[j].start()
        emit(col)
        if j:
            cf[j - 1].wait_recv()
            emit(pl.multiple_of((1 - core) * HALF + (j - 1) * CW, CW))
    cf[NCH - 1].wait_recv()
    emit(pl.multiple_of((1 - core) * HALF + (NCH - 1) * CW, CW))
    for j in range(NCH):
        ca[j].wait_send()
        cx[j].wait_send()
        cf[j].wait_send()


def reduce_scratch(slots):
    chunk = pltpu.VMEM((NCH, 64, CW), F32)
    return [pltpu.VMEM((64, 2 * HALF), F32), chunk, chunk, chunk, chunk, pltpu.VMEM((slots, 1024, CW), BF16),
            pltpu.SemaphoreType.DMA((6, NCH)), pltpu.SemaphoreType.DMA((slots,))]


NAB = 8
DA = 128


def k2_body(o_in, gate_in, h1, onorm, w_out, g2, wattn, clen, alpha, beta, vc,
            h2_out, qs, kn, vn, vpre,
            full, send_a, recv_a, own, recv_x, wo, sems, wosem,
            xin, ssl, ssr, sssem, abuf, ascr, wd, asem, cosf, sina, sinb, vsem):
    tp = lax.axis_index('tp')
    nchunk = h1.shape[1] // DA
    wcopies = out_weight_copies(w_out, wo, wosem)
    for c in wcopies[:wo.shape[0]]:
        c.start()

    def acopy(i, slot):
        return pltpu.make_async_copy(wattn.at[pl.ds(i * (DA * 12), DA * 12)], abuf.at[slot], asem.at[slot])
    for i in range(NAB):
        acopy(i, i).start()
    sq = jnp.zeros((64, 128), F32)
    for h in range(8):
        sq = sq + o_in[h] * o_in[h]
    wide = jnp.concatenate([sq, jnp.zeros((64, 128), F32)], axis=0).T
    ssl[...] = jnp.broadcast_to(jnp.sum(wide, axis=0, keepdims=True), (8, 128))
    entry_barrier()
    copies = [pltpu.make_async_remote_copy(src_ref=ssl, dst_ref=ssr.at[k], send_sem=sssem.at[0, k],
                                           recv_sem=sssem.at[1, k], device_id={'tp': dev}, device_id_type=MESH)
              for k, dev in enumerate(peers(tp))]
    for c in copies:
        c.start()
    def spread(b, carry):
        cosf[pl.ds(b, 1)] = jnp.full((1, 128), clen[b].astype(F32), F32)
        return carry

    lax.fori_loop(0, 64, spread, 0)
    lane = lax.broadcasted_iota(jnp.int32, (64, 128), 1)
    power = (lane & 31).astype(F32) * (-2.0 / 64)
    angle = cosf[...] * jnp.exp(power * math.log(ROPE_BASE))
    sine = jnp.sin(angle)
    cosf[...] = jnp.where(lane < 64, jnp.cos(angle), 1.0)
    sina[...] = jnp.where(lane < 32, -sine, 0.0)
    sinb[...] = jnp.where((lane >= 32) & (lane < 64), sine, 0.0)
    for c in copies:
        c.wait_recv()
    total = jnp.broadcast_to(((ssl[...] + ssr[0]) + (ssr[1] + ssr[2]))[0:1], (128, 128)).T[:64]
    inv = lax.rsqrt(total / 4096.0 + EPS)
    for h in range(8):
        xin[:, h * 128:(h + 1) * 128] = (o_in[h] * inv * onorm[h:h + 1] * gate_in[h]).astype(BF16)

    def demix(i, carry):
        slot = lax.rem(i, NAB)
        acopy(i, slot).wait()
        ascr[...] = abuf[slot].astype(F32)
        for j in range(6):
            for kv in range(2):
                wd[j, kv, pl.ds(pl.multiple_of(i * DA, DA), DA)] = ascr[pl.ds(2 * j + kv, DA, stride=12)].astype(BF16)

        @pl.when(i + NAB < nchunk)
        def _():
            acopy(i + NAB, slot).start()
        return carry

    vcopy = pltpu.make_async_copy(vc.at[pl.ds(0, NPRE * NB3)], vpre, vsem)

    def between(j):
        if j == 0:
            vcopy.start()
        lax.fori_loop(j * (nchunk // NCH), (j + 1) * (nchunk // NCH), demix, 0)

    reduce_over_tp(xin, wo, wcopies, full, send_a, recv_a, own, recv_x, sems, between, lambda col: None)
    for c in copies:
        c.wait_send()
    vcopy.wait()
    mid = (alpha[0] * h1[...].astype(F32) + beta[0] * full[...]).astype(BF16).astype(F32)
    h2_out[...] = (mid * lax.rsqrt(jnp.mean(mid * mid, axis=-1, keepdims=True) + EPS) * g2[...]).astype(BF16)
    qs[...] = jnp.zeros_like(qs)

    def turn(z):
        return z * cosf[...] + pltpu.roll(z, 96, 1) * sina[...] + pltpu.roll(z, 32, 1) * sinb[...]

    for j in range(6):
        r = jnp.concatenate([wd[j, 0], wd[j, 1]], axis=1)
        z = jnp.dot(h2_out[...], r, preferred_element_type=F32)
        for kv in range(2):
            zk = z[:, kv * 128:(kv + 1) * 128]
            if j < 4:
                qs[kv, pl.ds(kv * 4 + j, 64, stride=8)] = turn(zk).astype(BF16).astype(F32)
            elif j == 4:
                kn[kv] = turn(zk).astype(BF16).astype(F32)
            else:
                vn[kv] = zk.astype(BF16).astype(F32)


def k2(o, gate, h1, onorm, w_out, g2, wattn, clen, alpha, beta, vc):
    return pl.pallas_call(
        k2_body,
        out_shape=(jax.ShapeDtypeStruct(h1.shape, BF16), jax.ShapeDtypeStruct((2, 512, 128), F32),
                   jax.ShapeDtypeStruct((2, 64, 128), F32), jax.ShapeDtypeStruct((2, 64, 128), F32),
                   jax.ShapeDtypeStruct((NPRE * NB3,) + vc.shape[1:], BF16)),
        in_specs=[VMEM, VMEM, VMEM, VMEM, HBM, VMEM, HBM, SMEM, SMEM, SMEM, HBM],
        out_specs=(VMEM,) * 5,
        scratch_shapes=reduce_scratch(4) + [
            pltpu.VMEM((64, 1024), BF16), pltpu.VMEM((8, 128), F32), pltpu.VMEM((3, 8, 128), F32),
            pltpu.SemaphoreType.DMA((2, 3)),
            pltpu.VMEM((NAB, DA * 12, 128), BF16), pltpu.VMEM((DA * 12, 128), F32),
            pltpu.VMEM((6, 2, h1.shape[1], 128), BF16), pltpu.SemaphoreType.DMA((NAB,)),
            pltpu.VMEM((64, 128), F32), pltpu.VMEM((64, 128), F32), pltpu.VMEM((64, 128), F32),
            pltpu.SemaphoreType.DMA],
        compiler_params=pltpu.CompilerParams(vmem_limit_bytes=29 * 2 ** 20, collective_id=0, has_side_effects=True),
        cost_estimate=pl.CostEstimate(flops=int(6e10), bytes_accessed=int(2e7), transcendentals=0),
        name='mix_first')(o, gate, h1, onorm, w_out, g2, wattn, clen, alpha, beta, vc)


def k3_body(kc, vc, vpre, qs, kn, vn, clen, k_out, v_out, attn, kb, vb, sscr, rsem, wsem):
    nstep = kc.shape[0] // NB3

    def reads(i, slot):
        return (pltpu.make_async_copy(vc.at[pl.ds(i * NB3, NB3)], vb.at[slot], rsem.at[slot, 1]),)

    def writes(i, slot):
        return (pltpu.make_async_copy(kb.at[slot], k_out.at[pl.ds(i * NB3, NB3)], wsem.at[slot, 0]),
                pltpu.make_async_copy(vb.at[slot], v_out.at[pl.ds(i * NB3, NB3)], wsem.at[slot, 1]))

    for i in range(NPRE, NS3):
        for c in reads(i, i):
            c.start()

    def step(i, carry):
        slot = lax.rem(i, NS3)

        @pl.when(i < NPRE)
        def _():
            vb[slot] = vpre[pl.ds(pl.multiple_of(jnp.minimum(i, NPRE - 1) * NB3, NB3), NB3)]

        @pl.when(i >= NPRE)
        def _():
            for c in reads(i, slot):
                c.wait()
        kb[slot] = kc[pl.ds(i * NB3, NB3)]
        row_id = lax.broadcasted_iota(jnp.int32, (16, 128), 0)
        for u in range(NB3):
            b = i * NB3 + u
            pos = clen[b]
            base = pl.multiple_of((pos // 16) * 16, 16)
            hit = row_id == pos - base
            for kv in range(2):
                for buf, new in ((kb, kn), (vb, vn)):
                    old = buf[slot, u, kv, pl.ds(base, 16)].astype(F32)
                    row = jnp.broadcast_to(new[kv, pl.ds(b, 1)], (16, 128))
                    buf[slot, u, kv, pl.ds(base, 16)] = jnp.where(hit, row, old).astype(BF16)
        for c in writes(i, slot):
            c.start()

        def score(h, carry):
            for u in range(NB3 // 2):
                w = h * (NB3 // 2) + u
                b = i * NB3 + w
                q = jnp.concatenate([qs[0, pl.ds(b * 8, 8)], qs[1, pl.ds(b * 8, 8)]], axis=1).astype(BF16)
                both = jnp.concatenate([kb[slot, w, 0], kb[slot, w, 1]], axis=1)
                s = lax.dot_general(q, both, (((1,), (1,)), ((), ())), preferred_element_type=F32)
                sscr[w] = s * (128 ** -0.5)
            return carry

        lax.fori_loop(0, 2, score, 0)
        tpos = lax.broadcasted_iota(jnp.int32, (8, 512), 1)
        for w in range(NB3):
            s = jnp.where(tpos <= clen[i * NB3 + w], sscr[w], -jnp.inf)
            e = jnp.exp(s - jnp.max(s, axis=-1, keepdims=True))
            sscr[w] = (e / jnp.sum(e, axis=-1, keepdims=True)).astype(BF16).astype(F32)
        lo = lax.broadcasted_iota(jnp.int32, (8, 128), 0) < 4

        def weigh(h, carry):
            for u in range(NB3 // 2):
                w = h * (NB3 // 2) + u
                b = i * NB3 + w
                both = jnp.concatenate([vb[slot, w, 0], vb[slot, w, 1]], axis=1)
                r = jnp.dot(sscr[w].astype(BF16), both, preferred_element_type=F32)
                attn[pl.ds(b * 8, 8)] = jnp.where(lo, r[:, :128], r[:, 128:]).astype(BF16).astype(F32)
            return carry

        lax.fori_loop(0, 2, weigh, 0)
        nxt = i + NS3 - 1

        @pl.when((i >= 1) & (nxt < nstep))
        def _():
            ps = lax.rem(nxt, NS3)
            for c in writes(i - 1, ps):
                c.wait()
            for c in reads(nxt, ps):
                c.start()
        return carry

    lax.fori_loop(0, nstep, step, 0)
    for i in range(nstep - NS3, nstep):
        for c in writes(i, i % NS3):
            c.wait()


def k3(kc, vc, vpre, qs, kn, vn, clen):
    shape = (NS3, NB3) + kc.shape[1:]
    return pl.pallas_call(
        k3_body,
        out_shape=(jax.ShapeDtypeStruct(kc.shape, BF16), jax.ShapeDtypeStruct(vc.shape, BF16),
                   jax.ShapeDtypeStruct((512, 128), F32)),
        in_specs=[VMEM, HBM, VMEM, VMEM, VMEM, VMEM, SMEM],
        out_specs=(ANY, ANY, VMEM),
        scratch_shapes=[pltpu.VMEM(shape, BF16), pltpu.VMEM(shape, BF16), pltpu.VMEM((NB3, 8, 512), F32),
                        pltpu.SemaphoreType.DMA((NS3, 2)), pltpu.SemaphoreType.DMA((NS3, 2))],
        compiler_params=pltpu.CompilerParams(vmem_limit_bytes=24 * 2 ** 20),
        cost_estimate=pl.CostEstimate(flops=int(1e9), bytes_accessed=int(6e7), transcendentals=0),
        name='attention')(kc, vc, vpre, qs, kn, vn, clen)


def k4_body(attn, h2, w_out, alpha, beta, out,
            full, send_a, recv_a, own, recv_x, wo, sems, wosem, xin):
    wcopies = out_weight_copies(w_out, wo, wosem)
    for c in wcopies[:wo.shape[0]]:
        c.start()
    for r in range(8):
        xin[:, r * 128:(r + 1) * 128] = attn[pl.ds(r, 64, stride=8)].astype(BF16)
    entry_barrier()

    def emit(col):
        cols = pl.ds(col, CW)
        out[:, cols] = (alpha[1] * h2[:, cols].astype(F32) + beta[1] * full[:, cols]).astype(BF16)

    reduce_over_tp(xin, wo, wcopies, full, send_a, recv_a, own, recv_x, sems, lambda j: None, emit)


def k4(attn, h2, w_out, alpha, beta):
    return pl.pallas_call(
        k4_body,
        out_shape=jax.ShapeDtypeStruct(h2.shape, BF16),
        in_specs=[VMEM, VMEM, HBM, SMEM, SMEM],
        out_specs=VMEM,
        scratch_shapes=reduce_scratch(2 * NCH) + [pltpu.VMEM((64, 1024), BF16)],
        compiler_params=pltpu.CompilerParams(vmem_limit_bytes=20 * 2 ** 20, collective_id=1, has_side_effects=True),
        cost_estimate=pl.CostEstimate(flops=int(2e10), bytes_accessed=int(2e6), transcendentals=0),
        name='mix_second')(attn, h2, w_out, alpha, beta)


def solution(mesh):
    row_spec = P('dp', None)
    cache_spec = P('dp', 'tp', None, None)
    in_specs = (row_spec, P('dp'), cache_spec, cache_spec, cache_spec, P(None), P(None, None, 'tp', None),
                P(None, 'tp', None), P('tp'), P('tp', None), P('tp', None, None), P(None),
                P(None, 'tp', None, None), P('tp', None, None), P(None), P(None))
    out_specs = (row_spec, cache_spec, cache_spec, cache_spec)

    def local_step(hidden, cache_len, lin_state, k_cache, v_cache, norm_first, w_qkv, w_gate, slopes, out_norm,
                   w_out_lin, norm_second, w_attn, w_out_attn, mix_alpha, mix_beta):
        d = hidden.shape[1]

        def pin(x):
            return pltpu.with_memory_space_constraint(x, pltpu.HBM)
        state_out, o, gate, h1 = k1(pin(hidden), pin(norm_first.reshape(1, d)), pin(w_qkv.reshape(-1, 128)),
                                    pin(w_gate.reshape(-1, 128)), pin(slopes), pin(lin_state))
        pinned_v = pin(v_cache)
        wattn = pin(jnp.transpose(w_attn, (0, 2, 1, 3)).reshape(-1, 128))
        h2, qs, kn, vn, vpre = k2(o, gate, h1, out_norm, pin(w_out_lin.reshape(-1, d)), norm_second.reshape(1, d), wattn,
                            cache_len, mix_alpha, mix_beta, pinned_v)
        k_out, v_out, attn = k3(k_cache, pinned_v, vpre, qs, kn, vn, cache_len)
        hidden_out = k4(attn, h2, pin(w_out_attn.reshape(-1, d)), mix_alpha, mix_beta)
        return hidden_out, state_out, k_out, v_out

    return jax.shard_map(local_step, mesh=mesh, in_specs=in_specs, out_specs=out_specs, check_vma=False)
```

```python
import math
import jax
import jax.numpy as jnp
from jax import lax
from jax.experimental import pallas as pl
from jax.experimental.pallas import tpu as pltpu
from jax.sharding import PartitionSpec as P

EPS = 1e-5
ROPE_BASE = 10000000.0
F32 = jnp.float32
BF16 = jnp.bfloat16
MESH = pl.DeviceIdType.MESH
ANY = pl.BlockSpec(memory_space=pl.ANY)
HBM = pl.BlockSpec(memory_space=pltpu.HBM)
VMEM = pl.BlockSpec(memory_space=pltpu.VMEM)
SMEM = pl.BlockSpec(memory_space=pltpu.SMEM)

DC = 256
RS = 9 * DC + 16
NWB = 5
NSB = 23
LAG = 2
LATE = 17


def k1_body(hid_hbm, g1_hbm, wqkv, wgate, slopes_hbm, lin, st_out, o_out, gate_out, h1_out,
            wbuf, gbuf, scr, acc, qq, kk, vv, sbuf, hid, g1, slopes, wsem, rsem, ssem, msem):
    nchunk = hid.shape[1] // DC
    small = [pltpu.make_async_copy(src, dst, msem.at[n])
             for n, (src, dst) in enumerate(((hid_hbm, hid), (g1_hbm, g1), (slopes_hbm, slopes)))]
    for c in small:
        c.start()

    def wcopies(i, slot):
        return (pltpu.make_async_copy(wqkv.at[pl.ds(i * (DC * 24), DC * 24)], wbuf.at[slot], wsem.at[slot, 0]),
                pltpu.make_async_copy(wgate.at[pl.ds(i * (DC * 8), DC * 8)], gbuf.at[slot], wsem.at[slot, 1]))

    def sread(j, slot):
        hp, bb = j // 8, lax.rem(j, 8)
        return pltpu.make_async_copy(lin.at[pl.ds(bb * 8, 8), pl.ds(hp * 2, 2)], sbuf.at[slot], rsem.at[slot])

    def swrite(j, slot):
        hp, bb = j // 8, lax.rem(j, 8)
        return pltpu.make_async_copy(sbuf.at[slot], st_out.at[pl.ds(bb * 8, 8), pl.ds(hp * 2, 2)], ssem.at[slot])

    for i in range(NWB):
        for c in wcopies(i, i):
            c.start()
    for c in small:
        c.wait()
    x = hid[...].astype(F32)
    h1_out[...] = (x * lax.rsqrt(jnp.mean(x * x, axis=-1, keepdims=True) + EPS) * g1[...]).astype(BF16)
    acc[...] = jnp.zeros_like(acc)

    def wstep(i, carry):
        slot = lax.rem(i, NWB)
        for c in wcopies(i, slot):
            c.wait()
        for d2 in range(0, DC, 2):
            t = wbuf[slot, pl.ds(d2 * 24, 48)].astype(F32)
            for u in range(6):
                scr[pl.ds((u % 3) * RS + 9 * (d2 + u // 3), 8, stride=2)] = t[u * 8:(u + 1) * 8]
            t = gbuf[slot, pl.ds(d2 * 8, 16)].astype(F32)
            for u in range(2):
                scr[pl.ds(3 * RS + 9 * (d2 + u), 8, stride=2)] = t[u * 8:(u + 1) * 8]
        hh = h1_out[:, pl.ds(pl.multiple_of(i * DC, DC), DC)]

        def head(m):
            return scr[pl.ds((m // 8) * RS + 2 * (m % 8), DC, stride=9)]

        for n in range(16):
            r = jnp.concatenate([head(2 * n), head(2 * n + 1)], axis=1).astype(BF16)
            acc[:, n * 256:(n + 1) * 256] += jnp.dot(hh, r, preferred_element_type=F32)

        @pl.when(i + NWB < nchunk)
        def _():
            for c in wcopies(i + NWB, slot):
                c.start()

        sread(i, i).start()

        @pl.when(i >= LATE)
        def _():
            sread(i - LATE + nchunk, i - LATE + nchunk).start()
        return carry

    lax.fori_loop(0, nchunk, wstep, 0)

    for hp in range(4):
        def pair(c):
            base = c * 1024 + hp * 256
            return jnp.concatenate([acc[:, base:base + 128], acc[:, base + 128:base + 256]], axis=0)

        def act(c):
            z = pair(c)
            return (z * jax.nn.sigmoid(z)).astype(BF16).astype(F32)
        qq[hp] = act(0)
        kk[hp] = act(1)
        vv[hp] = act(2)
        g = jax.nn.sigmoid(pair(3))
        gate_out[2 * hp] = g[:64]
        gate_out[2 * hp + 1] = g[64:]

    def sstep(j, carry):
        hp, bb = j // 8, lax.rem(j, 8)
        slot = lax.rem(j, NSB)
        sread(j, slot).wait()
        rid = lax.broadcasted_iota(jnp.int32, (16, 128), 0)
        for p in range(2):
            decay = jnp.exp(jnp.full((8, 128), -slopes[hp * 2 + p], F32))[0:1]
            at = pl.ds(p * 64 + bb * 8, 8)
            kq = jnp.concatenate([kk[hp, at], qq[hp, at]], axis=0).T.astype(BF16)
            v16 = jnp.concatenate([vv[hp, at], jnp.zeros((8, 128), F32)], axis=0)
            rows = []
            for i in range(8):
                pick = jnp.concatenate([jnp.where(rid == i, v16, 0.0), jnp.where(rid == 8 + i, 1.0, 0.0)], axis=1)
                both = jnp.dot(kq, pick.astype(BF16), preferred_element_type=F32)
                s_new = decay * sbuf[slot, i, p] + both[:, :128]
                sbuf[slot, i, p] = s_new
                rows.append(jnp.sum(both[:, 128:] * s_new, axis=0, keepdims=True))
            o_out[hp * 2 + p, pl.ds(bb * 8, 8)] = jnp.concatenate(rows, axis=0)
        swrite(j, slot).start()

        @pl.when((j >= LAG) & (j - LAG + NSB < 32))
        def _():
            jj = j - LAG
            ps = lax.rem(jj, NSB)
            swrite(jj, ps).wait()
            sread(jj + NSB, ps).start()
        return carry

    lax.fori_loop(0, 32, sstep, 0)
    for j in range(32 - NSB, 32):
        swrite(j, j % NSB).wait()


def k1(hidden, g1, wqkv, wgate, slopes, lin):
    return pl.pallas_call(
        k1_body,
        out_shape=(jax.ShapeDtypeStruct(lin.shape, F32), jax.ShapeDtypeStruct((8, 64, 128), F32),
                   jax.ShapeDtypeStruct((8, 64, 128), F32), jax.ShapeDtypeStruct(hidden.shape, BF16)),
        in_specs=[HBM] * 6,
        out_specs=(ANY, VMEM, VMEM, VMEM),
        scratch_shapes=[
            pltpu.VMEM((NWB, DC * 24, 128), BF16), pltpu.VMEM((NWB, DC * 8, 128), BF16),
            pltpu.VMEM((4 * RS, 128), F32), pltpu.VMEM((64, 4096), F32),
            pltpu.VMEM((4, 128, 128), F32), pltpu.VMEM((4, 128, 128), F32), pltpu.VMEM((4, 128, 128), F32),
            pltpu.VMEM((NSB, 8, 2, 128, 128), F32),
            pltpu.VMEM(hidden.shape, BF16), pltpu.VMEM(g1.shape, F32), pltpu.SMEM(slopes.shape, F32),
            pltpu.SemaphoreType.DMA((NWB, 2)), pltpu.SemaphoreType.DMA((NSB,)), pltpu.SemaphoreType.DMA((NSB,)),
            pltpu.SemaphoreType.DMA((3,))],
        compiler_params=pltpu.CompilerParams(vmem_limit_bytes=45 * 2 ** 20),
        cost_estimate=pl.CostEstimate(flops=int(1e12), bytes_accessed=int(1.1e8), transcendentals=0),
        name='lightning')(hidden, g1, wqkv, wgate, slopes, lin)


NB3 = 8
NS3 = 4
NPRE = 3

NCH = 5
CW = 512
HALF = NCH * CW


def entry_barrier():
    tp = lax.axis_index('tp')
    bar = pltpu.get_barrier_semaphore()
    for peer in peers(tp):
        pl.semaphore_signal(bar, inc=1, device_id={'tp': peer}, device_id_type=MESH)
    pl.semaphore_wait(bar, 3)


def peers(tp):
    core = lax.rem(tp, 2)
    partner = tp + 1 - 2 * core
    across = lax.rem(tp + 2, 4)
    diag = lax.rem(partner + 2, 4)
    return partner, across, diag


def out_weight_copies(w, wo, wosem):
    core = lax.rem(lax.axis_index('tp'), 2)
    out = []
    for s in range(2 * NCH):
        side = core if s % 2 else 1 - core
        col = pl.multiple_of(side * HALF + (s // 2) * CW, CW)
        slot = s % wo.shape[0]
        out.append(pltpu.make_async_copy(w.at[:, pl.ds(col, CW)], wo.at[slot], wosem.at[slot]))
    return out


def reduce_over_tp(xin, wo, wcopies, full, send_a, recv_a, own, recv_x, sems, between, emit):
    tp = lax.axis_index('tp')
    core = lax.rem(tp, 2)
    partner, across, _ = peers(tp)

    def rcopy(src, dst, k, j, dev):
        return pltpu.make_async_remote_copy(src_ref=src, dst_ref=dst, send_sem=sems.at[k, j],
                                            recv_sem=sems.at[k + 1, j], device_id={'tp': dev}, device_id_type=MESH)
    ca = [rcopy(send_a.at[j], recv_a.at[j], 0, j, partner) for j in range(NCH)]
    cx = [rcopy(own.at[j], recv_x.at[j], 2, j, across) for j in range(NCH)]
    cf = []
    for j in range(NCH):
        col = pl.multiple_of(core * HALF + j * CW, CW)
        cf.append(rcopy(full.at[:, pl.ds(col, CW)], full.at[:, pl.ds(col, CW)], 4, j, partner))

    def product(n):
        wcopies[n].wait()
        out = jnp.dot(xin[...], wo[n % wo.shape[0]], preferred_element_type=F32)
        if n + wo.shape[0] < 2 * NCH:
            wcopies[n + wo.shape[0]].start()
        return out

    def combine(j):
        ca[j].wait_recv()
        own[j] = own[j] + recv_a[j]
        cx[j].start()

    for j in range(NCH):
        send_a[j] = product(2 * j)
        ca[j].start()
        own[j] = product(2 * j + 1)
        if j:
            combine(j - 1)
    combine(NCH - 1)
    for j in range(NCH):
        between(j)
        cx[j].wait_recv()
        col = pl.multiple_of(core * HALF + j * CW, CW)
        full[:, pl.ds(col, CW)] = own[j] + recv_x[j]
        cf[j].start()
        emit(col)
        if j:
            cf[j - 1].wait_recv()
            emit(pl.multiple_of((1 - core) * HALF + (j - 1) * CW, CW))
    cf[NCH - 1].wait_recv()
    emit(pl.multiple_of((1 - core) * HALF + (NCH - 1) * CW, CW))
    for j in range(NCH):
        ca[j].wait_send()
        cx[j].wait_send()
        cf[j].wait_send()


def reduce_scratch(slots):
    chunk = pltpu.VMEM((NCH, 64, CW), F32)
    return [pltpu.VMEM((64, 2 * HALF), F32), chunk, chunk, chunk, chunk, pltpu.VMEM((slots, 1024, CW), BF16),
            pltpu.SemaphoreType.DMA((6, NCH)), pltpu.SemaphoreType.DMA((slots,))]


NAB = 8
DA = 128


def k2_body(o_in, gate_in, h1, onorm, w_out, g2, wattn, clen, alpha, beta, vc,
            h2_out, qs, kn, vn, vpre,
            full, send_a, recv_a, own, recv_x, wo, sems, wosem,
            xin, ssl, ssr, sssem, abuf, ascr, wd, asem, cosf, sina, sinb, vsem):
    tp = lax.axis_index('tp')
    nchunk = h1.shape[1] // DA
    wcopies = out_weight_copies(w_out, wo, wosem)
    for c in wcopies[:wo.shape[0]]:
        c.start()

    def acopy(i, slot):
        return pltpu.make_async_copy(wattn.at[pl.ds(i * (DA * 12), DA * 12)], abuf.at[slot], asem.at[slot])
    for i in range(NAB):
        acopy(i, i).start()
    sq = jnp.zeros((64, 128), F32)
    for h in range(8):
        sq = sq + o_in[h] * o_in[h]
    wide = jnp.concatenate([sq, jnp.zeros((64, 128), F32)], axis=0).T
    ssl[...] = jnp.broadcast_to(jnp.sum(wide, axis=0, keepdims=True), (8, 128))
    entry_barrier()
    copies = [pltpu.make_async_remote_copy(src_ref=ssl, dst_ref=ssr.at[k], send_sem=sssem.at[0, k],
                                           recv_sem=sssem.at[1, k], device_id={'tp': dev}, device_id_type=MESH)
              for k, dev in enumerate(peers(tp))]
    for c in copies:
        c.start()
    def spread(b, carry):
        cosf[pl.ds(b, 1)] = jnp.full((1, 128), clen[b].astype(F32), F32)
        return carry

    lax.fori_loop(0, 64, spread, 0)
    lane = lax.broadcasted_iota(jnp.int32, (64, 128), 1)
    power = (lane & 31).astype(F32) * (-2.0 / 64)
    angle = cosf[...] * jnp.exp(power * math.log(ROPE_BASE))
    sine = jnp.sin(angle)
    cosf[...] = jnp.where(lane < 64, jnp.cos(angle), 1.0)
    sina[...] = jnp.where(lane < 32, -sine, 0.0)
    sinb[...] = jnp.where((lane >= 32) & (lane < 64), sine, 0.0)
    for c in copies:
        c.wait_recv()
    total = jnp.broadcast_to(((ssl[...] + ssr[0]) + (ssr[1] + ssr[2]))[0:1], (128, 128)).T[:64]
    inv = lax.rsqrt(total / 4096.0 + EPS)
    for h in range(8):
        xin[:, h * 128:(h + 1) * 128] = (o_in[h] * inv * onorm[h:h + 1] * gate_in[h]).astype(BF16)

    def demix(i, carry):
        slot = lax.rem(i, NAB)
        acopy(i, slot).wait()
        ascr[...] = abuf[slot].astype(F32)
        for j in range(6):
            for kv in range(2):
                wd[j, kv, pl.ds(pl.multiple_of(i * DA, DA), DA)] = ascr[pl.ds(2 * j + kv, DA, stride=12)].astype(BF16)

        @pl.when(i + NAB < nchunk)
        def _():
            acopy(i + NAB, slot).start()
        return carry

    vcopy = pltpu.make_async_copy(vc.at[pl.ds(0, NPRE * NB3)], vpre, vsem)

    def between(j):
        if j == 0:
            vcopy.start()
        lax.fori_loop(j * (nchunk // NCH), (j + 1) * (nchunk // NCH), demix, 0)

    def emit(col):
        cols = pl.ds(col, CW)
        h2_out[:, cols] = (alpha[0] * h1[:, cols].astype(F32) + beta[0] * full[:, cols]).astype(BF16)

    reduce_over_tp(xin, wo, wcopies, full, send_a, recv_a, own, recv_x, sems, between, emit)
    for c in copies:
        c.wait_send()
    vcopy.wait()
    mid = h2_out[...].astype(F32)
    h2_out[...] = (mid * lax.rsqrt(jnp.mean(mid * mid, axis=-1, keepdims=True) + EPS) * g2[...]).astype(BF16)
    qs[...] = jnp.zeros_like(qs)

    def turn(z):
        return z * cosf[...] + pltpu.roll(z, 96, 1) * sina[...] + pltpu.roll(z, 32, 1) * sinb[...]

    for j in range(6):
        r = jnp.concatenate([wd[j, 0], wd[j, 1]], axis=1)
        z = jnp.dot(h2_out[...], r, preferred_element_type=F32)
        for kv in range(2):
            zk = z[:, kv * 128:(kv + 1) * 128]
            if j < 4:
                qs[kv, pl.ds(kv * 4 + j, 64, stride=8)] = turn(zk).astype(BF16).astype(F32)
            elif j == 4:
                kn[kv] = turn(zk).astype(BF16).astype(F32)
            else:
                vn[kv] = zk.astype(BF16).astype(F32)


def k2(o, gate, h1, onorm, w_out, g2, wattn, clen, alpha, beta, vc):
    return pl.pallas_call(
        k2_body,
        out_shape=(jax.ShapeDtypeStruct(h1.shape, BF16), jax.ShapeDtypeStruct((2, 512, 128), F32),
                   jax.ShapeDtypeStruct((2, 64, 128), F32), jax.ShapeDtypeStruct((2, 64, 128), F32),
                   jax.ShapeDtypeStruct((NPRE * NB3,) + vc.shape[1:], BF16)),
        in_specs=[VMEM, VMEM, VMEM, VMEM, HBM, VMEM, HBM, SMEM, SMEM, SMEM, HBM],
        out_specs=(VMEM,) * 5,
        scratch_shapes=reduce_scratch(4) + [
            pltpu.VMEM((64, 1024), BF16), pltpu.VMEM((8, 128), F32), pltpu.VMEM((3, 8, 128), F32),
            pltpu.SemaphoreType.DMA((2, 3)),
            pltpu.VMEM((NAB, DA * 12, 128), BF16), pltpu.VMEM((DA * 12, 128), F32),
            pltpu.VMEM((6, 2, h1.shape[1], 128), BF16), pltpu.SemaphoreType.DMA((NAB,)),
            pltpu.VMEM((64, 128), F32), pltpu.VMEM((64, 128), F32), pltpu.VMEM((64, 128), F32),
            pltpu.SemaphoreType.DMA],
        compiler_params=pltpu.CompilerParams(vmem_limit_bytes=29 * 2 ** 20, collective_id=0, has_side_effects=True),
        cost_estimate=pl.CostEstimate(flops=int(6e10), bytes_accessed=int(2e7), transcendentals=0),
        name='mix_first')(o, gate, h1, onorm, w_out, g2, wattn, clen, alpha, beta, vc)


def k3_body(kc, vc, vpre, qs, kn, vn, clen, k_out, v_out, attn, kb, vb, sscr, rsem, wsem):
    nstep = kc.shape[0] // NB3

    def reads(i, slot):
        return (pltpu.make_async_copy(vc.at[pl.ds(i * NB3, NB3)], vb.at[slot], rsem.at[slot, 1]),)

    def writes(i, slot):
        return (pltpu.make_async_copy(kb.at[slot], k_out.at[pl.ds(i * NB3, NB3)], wsem.at[slot, 0]),
                pltpu.make_async_copy(vb.at[slot], v_out.at[pl.ds(i * NB3, NB3)], wsem.at[slot, 1]))

    for i in range(NPRE, NS3):
        for c in reads(i, i):
            c.start()

    def step(i, carry):
        slot = lax.rem(i, NS3)

        @pl.when(i < NPRE)
        def _():
            vb[slot] = vpre[pl.ds(pl.multiple_of(jnp.minimum(i, NPRE - 1) * NB3, NB3), NB3)]

        @pl.when(i >= NPRE)
        def _():
            for c in reads(i, slot):
                c.wait()
        kb[slot] = kc[pl.ds(i * NB3, NB3)]
        row_id = lax.broadcasted_iota(jnp.int32, (16, 128), 0)
        for u in range(NB3):
            b = i * NB3 + u
            pos = clen[b]
            base = pl.multiple_of((pos // 16) * 16, 16)
            hit = row_id == pos - base
            for kv in range(2):
                for buf, new in ((kb, kn), (vb, vn)):
                    old = buf[slot, u, kv, pl.ds(base, 16)].astype(F32)
                    row = jnp.broadcast_to(new[kv, pl.ds(b, 1)], (16, 128))
                    buf[slot, u, kv, pl.ds(base, 16)] = jnp.where(hit, row, old).astype(BF16)
        for c in writes(i, slot):
            c.start()

        def score(h, carry):
            for u in range(NB3 // 2):
                w = h * (NB3 // 2) + u
                b = i * NB3 + w
                q = jnp.concatenate([qs[0, pl.ds(b * 8, 8)], qs[1, pl.ds(b * 8, 8)]], axis=1).astype(BF16)
                both = jnp.concatenate([kb[slot, w, 0], kb[slot, w, 1]], axis=1)
                s = lax.dot_general(q, both, (((1,), (1,)), ((), ())), preferred_element_type=F32)
                sscr[w] = s * (128 ** -0.5)
            return carry

        lax.fori_loop(0, 2, score, 0)
        tpos = lax.broadcasted_iota(jnp.int32, (8, 512), 1)
        for w in range(NB3):
            s = jnp.where(tpos <= clen[i * NB3 + w], sscr[w], -jnp.inf)
            e = jnp.exp(s - jnp.max(s, axis=-1, keepdims=True))
            sscr[w] = (e / jnp.sum(e, axis=-1, keepdims=True)).astype(BF16).astype(F32)
        lo = lax.broadcasted_iota(jnp.int32, (8, 128), 0) < 4

        def weigh(h, carry):
            for u in range(NB3 // 2):
                w = h * (NB3 // 2) + u
                b = i * NB3 + w
                both = jnp.concatenate([vb[slot, w, 0], vb[slot, w, 1]], axis=1)
                r = jnp.dot(sscr[w].astype(BF16), both, preferred_element_type=F32)
                attn[pl.ds(b * 8, 8)] = jnp.where(lo, r[:, :128], r[:, 128:]).astype(BF16).astype(F32)
            return carry

        lax.fori_loop(0, 2, weigh, 0)
        nxt = i + NS3 - 1

        @pl.when((i >= 1) & (nxt < nstep))
        def _():
            ps = lax.rem(nxt, NS3)
            for c in writes(i - 1, ps):
                c.wait()
            for c in reads(nxt, ps):
                c.start()
        return carry

    lax.fori_loop(0, nstep, step, 0)
    for i in range(nstep - NS3, nstep):
        for c in writes(i, i % NS3):
            c.wait()


def k3(kc, vc, vpre, qs, kn, vn, clen):
    shape = (NS3, NB3) + kc.shape[1:]
    return pl.pallas_call(
        k3_body,
        out_shape=(jax.ShapeDtypeStruct(kc.shape, BF16), jax.ShapeDtypeStruct(vc.shape, BF16),
                   jax.ShapeDtypeStruct((512, 128), F32)),
        in_specs=[VMEM, HBM, VMEM, VMEM, VMEM, VMEM, SMEM],
        out_specs=(ANY, ANY, VMEM),
        scratch_shapes=[pltpu.VMEM(shape, BF16), pltpu.VMEM(shape, BF16), pltpu.VMEM((NB3, 8, 512), F32),
                        pltpu.SemaphoreType.DMA((NS3, 2)), pltpu.SemaphoreType.DMA((NS3, 2))],
        compiler_params=pltpu.CompilerParams(vmem_limit_bytes=24 * 2 ** 20),
        cost_estimate=pl.CostEstimate(flops=int(1e9), bytes_accessed=int(6e7), transcendentals=0),
        name='attention')(kc, vc, vpre, qs, kn, vn, clen)


def k4_body(attn, h2, w_out, alpha, beta, out,
            full, send_a, recv_a, own, recv_x, wo, sems, wosem, xin):
    wcopies = out_weight_copies(w_out, wo, wosem)
    for c in wcopies[:wo.shape[0]]:
        c.start()
    for r in range(8):
        xin[:, r * 128:(r + 1) * 128] = attn[pl.ds(r, 64, stride=8)].astype(BF16)
    entry_barrier()

    def emit(col):
        cols = pl.ds(col, CW)
        out[:, cols] = (alpha[1] * h2[:, cols].astype(F32) + beta[1] * full[:, cols]).astype(BF16)

    reduce_over_tp(xin, wo, wcopies, full, send_a, recv_a, own, recv_x, sems, lambda j: None, emit)


def k4(attn, h2, w_out, alpha, beta):
    return pl.pallas_call(
        k4_body,
        out_shape=jax.ShapeDtypeStruct(h2.shape, BF16),
        in_specs=[VMEM, VMEM, HBM, SMEM, SMEM],
        out_specs=VMEM,
        scratch_shapes=reduce_scratch(2 * NCH) + [pltpu.VMEM((64, 1024), BF16)],
        compiler_params=pltpu.CompilerParams(vmem_limit_bytes=20 * 2 ** 20, collective_id=1, has_side_effects=True),
        cost_estimate=pl.CostEstimate(flops=int(2e10), bytes_accessed=int(2e6), transcendentals=0),
        name='mix_second')(attn, h2, w_out, alpha, beta)


def solution(mesh):
    row_spec = P('dp', None)
    cache_spec = P('dp', 'tp', None, None)
    in_specs = (row_spec, P('dp'), cache_spec, cache_spec, cache_spec, P(None), P(None, None, 'tp', None),
                P(None, 'tp', None), P('tp'), P('tp', None), P('tp', None, None), P(None),
                P(None, 'tp', None, None), P('tp', None, None), P(None), P(None))
    out_specs = (row_spec, cache_spec, cache_spec, cache_spec)

    def local_step(hidden, cache_len, lin_state, k_cache, v_cache, norm_first, w_qkv, w_gate, slopes, out_norm,
                   w_out_lin, norm_second, w_attn, w_out_attn, mix_alpha, mix_beta):
        d = hidden.shape[1]

        def pin(x):
            return pltpu.with_memory_space_constraint(x, pltpu.HBM)
        state_out, o, gate, h1 = k1(pin(hidden), pin(norm_first.reshape(1, d)), pin(w_qkv.reshape(-1, 128)),
                                    pin(w_gate.reshape(-1, 128)), pin(slopes), pin(lin_state))
        pinned_v = pin(v_cache)
        wattn = pin(jnp.transpose(w_attn, (0, 2, 1, 3)).reshape(-1, 128))
        h2, qs, kn, vn, vpre = k2(o, gate, h1, out_norm, pin(w_out_lin.reshape(-1, d)), norm_second.reshape(1, d), wattn,
                            cache_len, mix_alpha, mix_beta, pinned_v)
        k_out, v_out, attn = k3(k_cache, pinned_v, vpre, qs, kn, vn, cache_len)
        hidden_out = k4(attn, h2, pin(w_out_attn.reshape(-1, d)), mix_alpha, mix_beta)
        return hidden_out, state_out, k_out, v_out

    return jax.shard_map(local_step, mesh=mesh, in_specs=in_specs, out_specs=out_specs, check_vma=False)
```
